32 devices in a mesh: data: 1 (over z), tensor: 32 (over y, x, core).
Axes of the slice: x: 4, y: 4, z: 1, core: 2. Of those that a mesh axis runs over, the one named last changes fastest.
The devices are a block of a 4x4x8 slice.
Arguments:
- x: bfloat16 [8, 1024, 4096], P('data')
- adapter_ids: int32 [8], P('data')
- norm_gain: float32 [4096], replicated
- w_query: bfloat16 [4096, 32, 128], P(None, 'tensor')
- w_key: bfloat16 [4096, 32, 128], P(None, 'tensor')
- w_value: bfloat16 [4096, 32, 128], P(None, 'tensor')
- w_out: bfloat16 [32, 128, 4096], P('tensor')
- w_gate: bfloat16 [4096, 16384], P(None, 'tensor')
- w_up: bfloat16 [4096, 16384], P(None, 'tensor')
- w_down: bfloat16 [16384, 4096], P('tensor')
- lora_a_query: bfloat16 [2, 4096, 128], P(None, None, 'tensor')
- lora_b_query: bfloat16 [2, 128, 32, 128], P(None, None, 'tensor')
- lora_a_key: bfloat16 [2, 4096, 128], P(None, None, 'tensor')
- lora_b_key: bfloat16 [2, 128, 32, 128], P(None, None, 'tensor')
- lora_a_value: bfloat16 [2, 4096, 128], P(None, None, 'tensor')
- lora_b_value: bfloat16 [2, 128, 32, 128], P(None, None, 'tensor')
- lora_a_out: bfloat16 [2, 32, 128, 128], P(None, 'tensor')
- lora_b_out: bfloat16 [2, 128, 4096], P(None, None, 'tensor')
- lora_a_gate: bfloat16 [2, 4096, 128], P(None, None, 'tensor')
- lora_b_gate: bfloat16 [2, 128, 16384], P(None, None, 'tensor')
- lora_a_up: bfloat16 [2, 4096, 128], P(None, None, 'tensor')
- lora_b_up: bfloat16 [2, 128, 16384], P(None, None, 'tensor')
- lora_a_down: bfloat16 [2, 16384, 128], P(None, 'tensor')
- lora_b_down: bfloat16 [2, 128, 4096], P(None, None, 'tensor')
Outputs:
- output: bfloat16 [8, 1024, 4096], P('data')
All inputs are finite; a program needn't handle non-finite values.
Results may differ from the reference program's by a relative error of at most 0.013888.
Values are sent between devices in bfloat16 or wider.
A program may use at most 768 MiB of HBM per device.

```python
import jax
import jax.numpy as jnp
import math
from jax import lax

SEQS = 8
SEQLEN = 1024
D = 4096
HEADS = 32
HEAD = 128
FF = 16384
R = 128
ADAPTERS = 2
ALPHA = 16

EPS = 1e-5
ROPE_BASE = 10000.0
SCALE = ALPHA / R
LORA_FRAC = 0.2


def normal_draw(key, shape, std):
    return (jax.random.normal(key, shape, jnp.float32) * std).astype(jnp.bfloat16)


def setup_inputs(seed: int = 0, part: int = 0) -> dict:
    root = jax.random.key(seed)
    part_key = jax.random.fold_in(root, part)
    x_key, id_key, slot_key = jax.random.split(part_key, 3)
    keys = jax.random.split(root, 22)
    hid_width = HEADS * HEAD
    qk_std = math.log(SEQLEN / 16.0) ** 0.25
    b_std = LORA_FRAC * math.sqrt(R) / ALPHA
    in_std = 1.0 / math.sqrt(D)
    adapter_ids = jax.random.randint(id_key, (SEQS,), 0, ADAPTERS, dtype=jnp.int32)
    slots = jax.random.permutation(slot_key, SEQS)
    adapter_ids = adapter_ids.at[slots[0]].set(ADAPTERS - 1).at[slots[1]].set(0)
    return {
        'x': normal_draw(x_key, (SEQS, SEQLEN, D), 1.0),
        'adapter_ids': adapter_ids,
        'norm_gain': 1.0 + 0.2 * jax.random.normal(keys[0], (D,), jnp.float32),
        'w_query': normal_draw(keys[1], (D, HEADS, HEAD), qk_std * in_std),
        'w_key': normal_draw(keys[2], (D, HEADS, HEAD), qk_std * in_std),
        'w_value': normal_draw(keys[3], (D, HEADS, HEAD), in_std),
        'w_out': normal_draw(keys[4], (HEADS, HEAD, D), 1.0 / math.sqrt(hid_width)),
        'w_gate': normal_draw(keys[5], (D, FF), in_std),
        'w_up': normal_draw(keys[6], (D, FF), in_std),
        'w_down': normal_draw(keys[7], (FF, D), 1.0 / math.sqrt(FF)),
        'lora_a_query': normal_draw(keys[8], (ADAPTERS, D, R), in_std),
        'lora_b_query': normal_draw(keys[9], (ADAPTERS, R, HEADS, HEAD), qk_std * b_std),
        'lora_a_key': normal_draw(keys[10], (ADAPTERS, D, R), in_std),
        'lora_b_key': normal_draw(keys[11], (ADAPTERS, R, HEADS, HEAD), qk_std * b_std),
        'lora_a_value': normal_draw(keys[12], (ADAPTERS, D, R), in_std),
        'lora_b_value': normal_draw(keys[13], (ADAPTERS, R, HEADS, HEAD), b_std),
        'lora_a_out': normal_draw(keys[14], (ADAPTERS, HEADS, HEAD, R), 1.0 / math.sqrt(hid_width)),
        'lora_b_out': normal_draw(keys[15], (ADAPTERS, R, D), b_std),
        'lora_a_gate': normal_draw(keys[16], (ADAPTERS, D, R), in_std),
        'lora_b_gate': normal_draw(keys[17], (ADAPTERS, R, FF), b_std),
        'lora_a_up': normal_draw(keys[18], (ADAPTERS, D, R), in_std),
        'lora_b_up': normal_draw(keys[19], (ADAPTERS, R, FF), b_std),
        'lora_a_down': normal_draw(keys[20], (ADAPTERS, FF, R), 1.0 / math.sqrt(FF)),
        'lora_b_down': normal_draw(keys[21], (ADAPTERS, R, D), b_std),
    }


def rope_rotate(vals, cos_t, sin_t):
    half_dim = vals.shape[-1] // 2
    first = vals[..., :half_dim]
    second = vals[..., half_dim:]
    return jnp.concatenate([first * cos_t - second * sin_t, second * cos_t + first * sin_t], axis=-1)


def lora_proj(rows_in, weight, a_stack, b_stack, adapter):
    base_out = jnp.dot(rows_in, weight, preferred_element_type=jnp.float32)
    lora_mid = jnp.dot(rows_in, a_stack[adapter], preferred_element_type=jnp.float32).astype(jnp.bfloat16)
    return base_out + SCALE * jnp.dot(lora_mid, b_stack[adapter], preferred_element_type=jnp.float32)


def reference(x, adapter_ids, norm_gain, w_query, w_key, w_value, w_out, w_gate, w_up, w_down, lora_a_query, lora_b_query, lora_a_key, lora_b_key, lora_a_value, lora_b_value, lora_a_out, lora_b_out, lora_a_gate, lora_b_gate, lora_a_up, lora_b_up, lora_a_down, lora_b_down):
    hid_width = HEADS * HEAD
    half_dim = HEAD // 2
    inv_freq = ROPE_BASE ** (-jnp.arange(half_dim, dtype=jnp.float32) / half_dim)
    angles = jnp.arange(SEQLEN, dtype=jnp.float32)[:, None] * inv_freq[None, :]
    cos_t = jnp.cos(angles)[:, None, :]
    sin_t = jnp.sin(angles)[:, None, :]
    causal = jnp.arange(SEQLEN)[:, None] >= jnp.arange(SEQLEN)[None, :]
    wq_flat = w_query.reshape(D, hid_width)
    wk_flat = w_key.reshape(D, hid_width)
    wv_flat = w_value.reshape(D, hid_width)
    wo_flat = w_out.reshape(hid_width, D)
    bq_flat = lora_b_query.reshape(ADAPTERS, R, hid_width)
    bk_flat = lora_b_key.reshape(ADAPTERS, R, hid_width)
    bv_flat = lora_b_value.reshape(ADAPTERS, R, hid_width)
    ao_flat = lora_a_out.reshape(ADAPTERS, hid_width, R)

    def one_sequence(seq_item):
        x_seq, adapter = seq_item
        x_f32 = x_seq.astype(jnp.float32)
        normed = (x_f32 * lax.rsqrt(jnp.mean(x_f32 * x_f32, axis=-1, keepdims=True) + EPS) * norm_gain).astype(jnp.bfloat16)
        z_query = lora_proj(normed, wq_flat, lora_a_query, bq_flat, adapter).reshape(SEQLEN, HEADS, HEAD)
        z_key = lora_proj(normed, wk_flat, lora_a_key, bk_flat, adapter).reshape(SEQLEN, HEADS, HEAD)
        z_value = lora_proj(normed, wv_flat, lora_a_value, bv_flat, adapter).reshape(SEQLEN, HEADS, HEAD)
        query_rot = rope_rotate(z_query, cos_t, sin_t).astype(jnp.bfloat16)
        key_rot = rope_rotate(z_key, cos_t, sin_t).astype(jnp.bfloat16)
        value_heads = z_value.astype(jnp.bfloat16)
        scores = jnp.einsum('qhd,khd->hqk', query_rot.astype(jnp.float32), key_rot.astype(jnp.float32)) / math.sqrt(HEAD)
        scores = jnp.where(causal[None], scores, -1e30)
        probs_bf = jax.nn.softmax(scores, axis=-1).astype(jnp.bfloat16)
        attended = jnp.einsum('hqk,khd->qhd', probs_bf.astype(jnp.float32), value_heads.astype(jnp.float32)).astype(jnp.bfloat16).reshape(SEQLEN, hid_width)
        z_out = lora_proj(attended, wo_flat, ao_flat, lora_b_out, adapter)
        gate_pre = lora_proj(normed, w_gate, lora_a_gate, lora_b_gate, adapter)
        up_pre = lora_proj(normed, w_up, lora_a_up, lora_b_up, adapter)
        mlp_mixed = (jax.nn.silu(gate_pre) * up_pre).astype(jnp.bfloat16)
        z_down = lora_proj(mlp_mixed, w_down, lora_a_down, lora_b_down, adapter)
        return (x_f32 + z_out + z_down).astype(jnp.bfloat16)

    return lax.map(one_sequence, (x, adapter_ids))
```

```python
import functools
import math

import jax
import jax.numpy as jnp
from jax import lax
from jax.experimental import pallas as pl
from jax.experimental.pallas import tpu as pltpu
from jax.sharding import PartitionSpec as P

ALPHA = 16
EPS = 1e-5
ROPE_BASE = 10000.0
MESH = pl.DeviceIdType.MESH
BF = jnp.bfloat16

def rms_norm(x_blk, norm_gain):
    x_f32 = x_blk.astype(jnp.float32)
    return (x_f32 * lax.rsqrt(jnp.mean(x_f32 * x_f32, axis=-1, keepdims=True) + EPS) * norm_gain).astype(jnp.bfloat16)


def rope_tables(seq_len, head_dim):
    half_dim = head_dim // 2
    inv_freq = ROPE_BASE ** (-jnp.arange(half_dim, dtype=jnp.float32) / half_dim)
    angles = jnp.arange(seq_len, dtype=jnp.float32)[:, None] * inv_freq[None, :]
    return jnp.cos(angles)[:, None, :], jnp.sin(angles)[:, None, :]


def rope_rotate(vals, cos_t, sin_t):
    half_dim = vals.shape[-1] // 2
    first = vals[..., :half_dim]
    second = vals[..., half_dim:]
    return jnp.concatenate([first * cos_t - second * sin_t, second * cos_t + first * sin_t], axis=-1)


def causal_attention(query_rot, key_rot, value_heads):
    seq_len = query_rot.shape[1]
    head_dim = query_rot.shape[3]
    scores = jnp.einsum('bqhd,bkhd->bhqk', query_rot, key_rot, preferred_element_type=jnp.float32) / math.sqrt(head_dim)
    causal = jnp.arange(seq_len)[:, None] >= jnp.arange(seq_len)[None, :]
    probs_bf = jax.nn.softmax(jnp.where(causal, scores, -1e30), axis=-1).astype(jnp.bfloat16)
    return jnp.einsum('bhqk,bkhd->bqhd', probs_bf, value_heads, preferred_element_type=jnp.float32).astype(jnp.bfloat16)


def comm_kernel(cfg, ids_ref, part_ref, midp_ref, x_ref, bod_ref, stage_ref,
                psend, pown, l0, r0, l1f, l1d, l1s, s1, r1, l2f, l2d, l2s, s2, r2, xrow, yrow, bodv,
                ld_sem, d2d_s, d2d_r, p1_s, p1_r, p2_s, p2_r, aga_s, aga_r, agb_s, agb_r, dd_s, dd_r, loc_sem):
    (N, R, NT, TT, W, D, scale, tiles_per_seq) = cfg
    HALF = TT // 2; B1 = HALF // R; B2 = B1 // R; WH = W // 2; DH = D // 2
    idx = lax.axis_index("tensor")
    c = lax.rem(idx, 2)
    xx = lax.rem(idx // 2, R)
    yy = idx // (2 * R)
    q1 = jnp.where(c == 0, xx, yy); q2 = jnp.where(c == 0, yy, xx)
    st1 = 2 + (2 * R - 2) * c; st2 = 2 * R - (2 * R - 2) * c
    b1 = idx - q1 * st1; b2 = idx - q2 * st2
    def nb(base, st, q, d): return base + lax.rem(q + d + R, R) * st
    plus1, minus1 = nb(b1, st1, q1, 1), nb(b1, st1, q1, -1)
    plus2, minus2 = nb(b2, st2, q2, 1), nb(b2, st2, q2, -1)
    mate = idx + 1 - 2 * c
    peers = (mate, plus1, minus1, plus2, minus2)

    bar = pltpu.get_barrier_semaphore()
    for p in peers:
        pl.semaphore_signal(bar, inc=1, device_id={"tensor": p}, device_id_type=MESH)
    pl.semaphore_wait(bar, len(peers))

    def rc(src, dst, ss, rs, dev):
        return pltpu.make_async_remote_copy(src_ref=src, dst_ref=dst, send_sem=ss, recv_sem=rs, device_id={"tensor": dev}, device_id_type=MESH)

    bcp = pltpu.make_async_copy(bod_ref, bodv, loc_sem.at[0])
    bcp.start(); bcp.wait()

    def blk(q, d, rows): return pl.ds(pl.multiple_of(lax.rem(q + d + R, R) * rows, rows), rows)
    A, B = pl.ds(0, WH), pl.ds(WH, WH)
    DA, DB = pl.ds(0, DH), pl.ds(DH, DH)

    def loads(t, half, buf, k):
        rows = pl.ds(pl.multiple_of(t * TT + half * HALF, HALF), HALF)
        return (pltpu.make_async_copy(part_ref.at[rows, :], buf.at[:, pl.ds(0, D)], ld_sem.at[k, 0]),
                pltpu.make_async_copy(midp_ref.at[rows, :], buf.at[:, pl.ds(D, W - D)], ld_sem.at[k, 1]))

    def d2d(t):
        s = lax.rem(t, 2)
        return rc(psend, l0.at[s], d2d_s, d2d_r.at[s], mate)
    def s1_copies(src, q, rows, lf, ld, ss, rs, plus, minus):
        return (rc(src.at[blk(q, 2, rows), A], lf.at[0], ss.at[0], rs.at[0], plus),
                rc(src.at[blk(q, 2, rows), B], lf.at[1], ss.at[1], rs.at[1], minus),
                rc(src.at[blk(q, 1, rows), B], ld.at[0], ss.at[2], rs.at[2], plus),
                rc(src.at[blk(q, -1, rows), A], ld.at[1], ss.at[3], rs.at[3], minus))
    def s2_copies(sm, ls, ss, rs, plus, minus):
        return (rc(sm.at[0], ls.at[0], ss.at[4], rs.at[4], plus),
                rc(sm.at[1], ls.at[1], ss.at[5], rs.at[5], minus))
    def p1s1(t): return s1_copies(r0, q1, B1, l1f, l1d, p1_s, p1_r, plus1, minus1)
    def p1s2(t): return s2_copies(s1, l1s, p1_s, p1_r, plus1, minus1)
    def p2s1(t):
        s = lax.rem(t, 2)
        return s1_copies(r1.at[s], q2, B2, l2f.at[s], l2d.at[s], p2_s.at[s], p2_r.at[s], plus2, minus2)
    def p2s2(t):
        s = lax.rem(t, 2)
        return s2_copies(s2, l2s.at[s], p2_s.at[s], p2_r.at[s], plus2, minus2)
    def row0(t): return t * TT + c * HALF
    def rows_a(t, d): return pl.ds(pl.multiple_of(row0(t) + q1 * B1 + lax.rem(q2 + d + R, R) * B2, B2), B2)
    def rows_b(t, d): return pl.ds(pl.multiple_of(row0(t) + lax.rem(q1 + d + R, R) * B1, B1), B1)
    def sl(t): return lax.rem(t, 4)
    def aga1(t):
        s = sl(t); r = rows_a(t, 0)
        return (rc(yrow, stage_ref.at[r, :], aga_s.at[s, 0], aga_r.at[s, 0], plus2),
                rc(yrow, stage_ref.at[r, :], aga_s.at[s, 1], aga_r.at[s, 1], minus2))
    def aga2(t):
        s = sl(t)
        return (rc(stage_ref.at[rows_a(t, -1), DA], stage_ref.at[rows_a(t, -1), DA], aga_s.at[s, 2], aga_r.at[s, 2], plus2),
                rc(stage_ref.at[rows_a(t, 1), DB], stage_ref.at[rows_a(t, 1), DB], aga_s.at[s, 3], aga_r.at[s, 3], minus2))
    def agb1(t):
        s = sl(t); r = rows_b(t, 0)
        return (rc(stage_ref.at[r, :], stage_ref.at[r, :], agb_s.at[s, 0], agb_r.at[s, 0], plus1),
                rc(stage_ref.at[r, :], stage_ref.at[r, :], agb_s.at[s, 1], agb_r.at[s, 1], minus1))
    def agb2(t):
        s = sl(t)
        return (rc(stage_ref.at[rows_b(t, -1), DA], stage_ref.at[rows_b(t, -1), DA], agb_s.at[s, 2], agb_r.at[s, 2], plus1),
                rc(stage_ref.at[rows_b(t, 1), DB], stage_ref.at[rows_b(t, 1), DB], agb_s.at[s, 3], agb_r.at[s, 3], minus1))
    def dd(t):
        s = sl(t); r = pl.ds(pl.multiple_of(row0(t), HALF), HALF)
        return rc(stage_ref.at[r, :], stage_ref.at[r, :], dd_s.at[s], dd_r.at[s], mate)
    def yloc(t): return pltpu.make_async_copy(yrow, stage_ref.at[rows_a(t, 0), :], loc_sem.at[1])
    def xload(t): return pltpu.make_async_copy(x_ref.at[rows_a(t, 0), :], xrow, loc_sem.at[2])

    def start(cs):
        for cp in cs: cp.start()
    def wrecv(cs):
        for cp in cs: cp.wait_recv()
    def wsend(cs):
        for cp in cs: cp.wait_send()

    def comb(src, q, rows, lf, ld, sm, dst):
        sm[0] = src[blk(q, 1, rows), A] + lf[0]
        sm[1] = src[blk(q, -1, rows), B] + lf[1]
        dst[:, A] = src[blk(q, 0, rows), A] + ld[1]
        dst[:, B] = src[blk(q, 0, rows), B] + ld[0]

    def e1(t):
        wrecv(p1s1(t)); wsend(p1s1(t))
        @pl.when(t >= 1)
        def _():
            wsend(p1s2(t - 1))
        comb(r0, q1, B1, l1f, l1d, s1, r1.at[lax.rem(t, 2)])
        start(p1s2(t))
    def e2(t):
        wrecv(p1s2(t))
        s = lax.rem(t, 2)
        r1[s, :, A] = r1[s, :, A] + l1s[0]
        r1[s, :, B] = r1[s, :, B] + l1s[1]
        start(p2s1(t))
    def e3(t):
        s = lax.rem(t, 2)
        wrecv(p2s1(t)); wsend(p2s1(t))
        @pl.when(t >= 1)
        def _(): wsend(p2s2(t - 1))
        comb(r1.at[s], q2, B2, l2f.at[s], l2d.at[s], s2, r2)
        start(p2s2(t))
        xload(t).start()
    def e4(t):
        s = lax.rem(t, 2)
        wrecv(p2s2(t))
        xload(t).wait()
        i = ids_ref[t // tiles_per_seq]
        r2[:, A] = r2[:, A] + l2s[s, 0]
        r2[:, B] = r2[:, B] + l2s[s, 1]
        mid = r2[:, pl.ds(D, W - D)]
        lor = jnp.dot(mid, bodv[i], preferred_element_type=jnp.float32)
        y = xrow[...].astype(jnp.float32) + r2[:, pl.ds(0, D)].astype(jnp.float32) + scale * lor
        yrow[...] = y.astype(BF)
        yloc(t).start()
        start(aga1(t))
    def e5(t):
        yloc(t).wait(); wsend(aga1(t)); wrecv(aga1(t)); start(aga2(t))
    def e6(t):
        wrecv(aga2(t)); start(agb1(t))
    def e7(t):
        wrecv(agb1(t)); start(agb2(t))
    def e8(t):
        wrecv(agb2(t)); start((dd(t),))
    def e9(t):
        wrecv((dd(t),)); wsend((dd(t),)); wsend(agb2(t)); wsend(agb1(t)); wsend(aga2(t))

    LAST = NT - 1
    def guard(t, f):
        @pl.when(jnp.logical_and(t >= 0, t < NT))
        def _(): f(t)

    for cp in loads(0, 1 - c, psend, 0) + loads(0, c, pown, 1): cp.start()

    def produce(t):
        for cp in loads(t, 1 - c, psend, 0): cp.wait()
        d2d(t).start()
        for cp in loads(t, c, pown, 1): cp.wait()
        d2d(t).wait_recv()
        r0[...] = pown[...] + l0[lax.rem(t, 2)]
        start(p1s1(t))
        d2d(t).wait_send()
        @pl.when(t + 1 < NT)
        def _():
            for cp in loads(t + 1, 1 - c, psend, 0) + loads(t + 1, c, pown, 1): cp.start()

    def body(it, _):
        guard(it - 1, e1)
        guard(it - 4, e7)
        guard(it - 2, e3)
        guard(it - 3, e5)
        guard(it - 1, e2)
        guard(it - 4, e8)
        guard(it - 2, e4)
        guard(it - 3, e6)
        guard(it - 5, e9)
        guard(it, produce)
        return 0
    lax.fori_loop(0, NT + 6, body, 0)
    wsend(p1s2(LAST)); wsend(p2s2(LAST));

def comm(mesh, part, midp, x, bod, ids, scale, tiles_per_seq, TT=512):
    N = mesh.shape["tensor"]; R = math.isqrt(N // 2)
    T, D = part.shape; W = D + midp.shape[1]
    NT = T // TT; HALF = TT // 2; B1 = HALF // R; B2 = B1 // R; WH = W // 2
    cfg = (N, R, NT, TT, W, D, scale, tiles_per_seq)
    V = pltpu.VMEM; S = pltpu.SemaphoreType.DMA
    return pl.pallas_call(
        functools.partial(comm_kernel, cfg), name="rsag",
        out_shape=jax.ShapeDtypeStruct((T, D), BF),
        in_specs=[pl.BlockSpec(memory_space=pltpu.SMEM)] + [pl.BlockSpec(memory_space=pl.ANY)] * 4,
        out_specs=pl.BlockSpec(memory_space=pl.ANY),
        scratch_shapes=[V((HALF, W), BF), V((HALF, W), BF), V((2, HALF, W), BF), V((HALF, W), BF),
                        V((2, B1, WH), BF), V((2, B1, WH), BF), V((2, B1, WH), BF), V((2, B1, WH), BF), V((2, B1, W), BF),
                        V((2, 2, B2, WH), BF), V((2, 2, B2, WH), BF), V((2, 2, B2, WH), BF), V((2, B2, WH), BF), V((B2, W), BF),
                        V((B2, D), BF), V((B2, D), BF), V(bod.shape, BF),
                        S((2, 2)), S, S((2,)), S((6,)), S((6,)), S((2, 6)), S((2, 6)), S((4, 4)), S((4, 4)), S((4, 4)), S((4, 4)), S((4,)), S((4,)), S((3,))],
        compiler_params=pltpu.CompilerParams(collective_id=0, has_side_effects=True, vmem_limit_bytes=60 * 2**20),
    )(ids, part, midp, x, bod)


def solution(mesh):
    batch_spec = P('data', None, None)
    head_cols = P(None, 'tensor', None)
    head_rows = P('tensor', None, None)
    ff_cols = P(None, 'tensor')
    ff_rows = P('tensor', None)
    last_split = P(None, None, 'tensor')
    b_heads = P(None, None, 'tensor', None)
    a_heads = P(None, 'tensor', None, None)
    in_specs = (batch_spec, P('data'), P(None), head_cols, head_cols, head_cols, head_rows, ff_cols, ff_cols, ff_rows, last_split, b_heads, last_split, b_heads, last_split, b_heads, a_heads, last_split, last_split, last_split, last_split, last_split, head_cols, last_split)

    def local_layer(x_blk, adapter_ids, norm_gain, w_query, w_key, w_value, w_out, w_gate, w_up, w_down, a_query, b_query, a_key, b_key, a_value, b_value, a_out, b_out, a_gate, b_gate, a_up, b_up, a_down, b_down):
        seq_len = x_blk.shape[1]
        rank = a_out.shape[-1]
        scale = ALPHA / rank
        normed = rms_norm(x_blk, norm_gain)
        cos_t, sin_t = rope_tables(seq_len, w_query.shape[-1])
        n_dev = mesh.shape['tensor']
        stacks = jnp.stack([a_query, a_key, a_value, a_gate, a_up])
        gathered = lax.all_gather(jnp.transpose(stacks, (1, 0, 3, 2)).reshape(-1, stacks.shape[2]), 'tensor', axis=0, tiled=True)
        gathered = gathered.reshape(n_dev, stacks.shape[1], stacks.shape[0], rank // n_dev, stacks.shape[2])
        a_all = jnp.transpose(gathered, (1, 2, 0, 3, 4)).reshape(stacks.shape[1], stacks.shape[0] * rank, stacks.shape[2])
        mids = jnp.einsum('bsd,brd->bsr', normed, a_all[adapter_ids], preferred_element_type=jnp.float32).astype(jnp.bfloat16)
        head = w_query.shape[-1]
        width = w_query.shape[1] * head
        w_in = jnp.concatenate([w.reshape(w.shape[0], -1) for w in (w_query, w_key, w_value, w_gate, w_up)], axis=1)

        def lora(k, b_stack):
            flat = b_stack.reshape(b_stack.shape[0], rank, -1)
            return scale * jnp.einsum('bsr,bre->bse', mids[:, :, k * rank:(k + 1) * rank], flat[adapter_ids], preferred_element_type=jnp.float32)

        base = jnp.einsum('bsd,de->bse', normed, w_in, preferred_element_type=jnp.float32)
        ff = w_gate.shape[1]
        heads = lambda k, b: (base[:, :, k * width:(k + 1) * width] + lora(k, b)).reshape(*x_blk.shape[:2], -1, head)
        query_rot = rope_rotate(heads(0, b_query), cos_t, sin_t).astype(jnp.bfloat16)
        key_rot = rope_rotate(heads(1, b_key), cos_t, sin_t).astype(jnp.bfloat16)
        value_heads = heads(2, b_value).astype(jnp.bfloat16)
        gate = base[:, :, 3 * width:3 * width + ff] + lora(3, b_gate)
        up = base[:, :, 3 * width + ff:] + lora(4, b_up)
        attended = causal_attention(query_rot, key_rot, value_heads)
        mlp_mixed = (jax.nn.silu(gate) * up).astype(jnp.bfloat16)
        mid_out = jnp.einsum('bshe,bher->bsr', attended, a_out[adapter_ids], preferred_element_type=jnp.float32)
        mid_down = jnp.einsum('bsf,bfr->bsr', mlp_mixed, a_down[adapter_ids], preferred_element_type=jnp.float32)
        mid_part = jnp.concatenate([mid_out, mid_down], axis=-1).astype(jnp.bfloat16)
        base_part = (jnp.einsum('bshe,hed->bsd', attended, w_out, preferred_element_type=jnp.float32) + jnp.einsum('bsf,fd->bsd', mlp_mixed, w_down, preferred_element_type=jnp.float32)).astype(jnp.bfloat16)
        b_both = lax.all_gather(jnp.concatenate([b_out, b_down], axis=1), 'tensor', axis=0)
        b_both = jnp.moveaxis(b_both, 0, 2).reshape(b_both.shape[1], b_both.shape[2], -1)
        seqs, _, width_out = x_blk.shape
        tile = seq_len // 2
        out = comm(mesh, base_part.reshape(-1, width_out), mid_part.reshape(-1, mid_part.shape[-1]), x_blk.reshape(-1, width_out), b_both, adapter_ids, scale, 2, tile)
        return out.reshape(x_blk.shape)

    return jax.shard_map(local_layer, mesh=mesh, in_specs=in_specs, out_specs=batch_spec, check_vma=False)
```

```python
import functools
import math

import jax
import jax.numpy as jnp
from jax import lax
from jax.experimental import pallas as pl
from jax.experimental.pallas import tpu as pltpu
from jax.sharding import PartitionSpec as P

ALPHA = 16
EPS = 1e-5
ROPE_BASE = 10000.0
MESH = pl.DeviceIdType.MESH
BF = jnp.bfloat16

def fused_kernel(cfg, ids_ref, x_ref, h_ref, at_ref, wq_ref, wk_ref, wv_ref, wg_ref, wu_ref, wo_ref, wd_ref, bqk_ref, bv_ref, bgu_ref,
                 aod_ref, bown_ref, cos_ref, sin_ref, stage_ref,
                 hbuf, mids, at_v, wqkv_v, wgu_v, wod_v, bqk_v, bv_v, bgu_v, aod_v, bod_v, cos_v, sin_v, qbuf, kbuf, vbuf, om,
                 psend, l0, r0, l1f, l1d, l1s, s1, r1, l2f, l2d, l2s, s2, r2, xrow, yrow,
                 w_sem, x_sem, d2d_s, d2d_r, p1_s, p1_r, p2_s, p2_r, aga_s, aga_r, agb_s, agb_r, dd_s, dd_r, bg_s, bg_r, loc_sem):
    R, NT, TT, W, D, HEAD, FF, scale, tps = cfg
    HALF = TT // 2
    B1 = HALF // R
    B2 = B1 // R
    WH = W // 2
    DH = D // 2
    KV = tps * TT
    FB = HALF
    idx = lax.axis_index("tensor")
    c = lax.rem(idx, 2)
    xx = lax.rem(idx // 2, R)
    yy = idx // (2 * R)
    q1 = jnp.where(c == 0, xx, yy)
    q2 = jnp.where(c == 0, yy, xx)
    st1 = 2 + (2 * R - 2) * c
    st2 = 2 * R - (2 * R - 2) * c
    base1 = idx - q1 * st1
    base2 = idx - q2 * st2
    plus1 = base1 + lax.rem(q1 + 1, R) * st1
    minus1 = base1 + lax.rem(q1 + R - 1, R) * st1
    plus2 = base2 + lax.rem(q2 + 1, R) * st2
    minus2 = base2 + lax.rem(q2 + R - 1, R) * st2
    mate = idx + 1 - 2 * c
    peers = (mate, plus1, minus1, plus2, minus2)

    resident = (
        ((at_ref, at_v),),
        ((wq_ref, wqkv_v.at[:, pl.ds(0, HEAD)]), (wk_ref, wqkv_v.at[:, pl.ds(HEAD, HEAD)]), (wv_ref, wqkv_v.at[:, pl.ds(2 * HEAD, HEAD)]),
         (bqk_ref, bqk_v), (bv_ref, bv_v), (cos_ref, cos_v), (sin_ref, sin_v)),
        ((wg_ref.at[:, pl.ds(0, FB)], wgu_v.at[:, pl.ds(0, FB)]), (wu_ref.at[:, pl.ds(0, FB)], wgu_v.at[:, pl.ds(FB, FB)]),
         (wg_ref.at[:, pl.ds(FB, FB)], wgu_v.at[:, pl.ds(2 * FB, FB)]), (wu_ref.at[:, pl.ds(FB, FB)], wgu_v.at[:, pl.ds(3 * FB, FB)]),
         (bgu_ref, bgu_v)),
        ((wo_ref, wod_v.at[pl.ds(0, HEAD), :]), (wd_ref, wod_v.at[pl.ds(HEAD, FF), :]), (aod_ref, aod_v)),
    )
    copies = []
    n_sem = 0
    for group in resident:
        row = []
        for src, dst in group:
            row.append(pltpu.make_async_copy(src, dst, w_sem.at[n_sem]))
            n_sem += 1
        copies.append(row)

    def xcopy(u):
        rows = pl.ds(pl.multiple_of(u * HALF, HALF), HALF)
        s = lax.rem(u, 2)
        return pltpu.make_async_copy(h_ref.at[rows, :], hbuf.at[s], x_sem.at[s])

    CB = bown_ref.shape[-1]

    def bcols(d):
        return pl.ds(pl.multiple_of(d * CB, CB), CB)

    bown = pltpu.make_async_copy(bown_ref, bod_v.at[:, :, bcols(idx)], loc_sem.at[2])
    xcopy(0).start()
    for row in copies:
        for cp in row:
            cp.start()

    bown.start()

    bar = pltpu.get_barrier_semaphore()
    for p in peers:
        pl.semaphore_signal(bar, inc=1, device_id={"tensor": p}, device_id_type=MESH)
    pl.semaphore_wait(bar, len(peers))
    vbuf[...] = jnp.zeros_like(vbuf)
    kbuf[...] = jnp.zeros_like(kbuf)

    def settle(t, hf, k):
        if hf == 0:
            @pl.when(t == 0)
            def _():
                for cp in copies[k]:
                    cp.wait()

    def rc(src, dst, ss, rs, dev):
        return pltpu.make_async_remote_copy(src_ref=src, dst_ref=dst, send_sem=ss, recv_sem=rs, device_id={"tensor": dev}, device_id_type=MESH)

    def blk(q, d, rows):
        return pl.ds(pl.multiple_of(lax.rem(q + d + R, R) * rows, rows), rows)

    A, B = pl.ds(0, WH), pl.ds(WH, WH)
    DA, DB = pl.ds(0, DH), pl.ds(DH, DH)

    def d2d(t):
        s = lax.rem(t, 2)
        return rc(psend, l0.at[s], d2d_s, d2d_r.at[s], mate)

    def first_copies(src, q, rows, lf, ld, ss, rs, plus, minus):
        return (rc(src.at[blk(q, 2, rows), A], lf.at[0], ss.at[0], rs.at[0], plus),
                rc(src.at[blk(q, 2, rows), B], lf.at[1], ss.at[1], rs.at[1], minus),
                rc(src.at[blk(q, 1, rows), B], ld.at[0], ss.at[2], rs.at[2], plus),
                rc(src.at[blk(q, -1, rows), A], ld.at[1], ss.at[3], rs.at[3], minus))

    def second_copies(sm, ls, ss, rs, plus, minus):
        return (rc(sm.at[0], ls.at[0], ss.at[4], rs.at[4], plus),
                rc(sm.at[1], ls.at[1], ss.at[5], rs.at[5], minus))

    def p1s1(t):
        return first_copies(r0, q1, B1, l1f, l1d, p1_s, p1_r, plus1, minus1)

    def p1s2(t):
        return second_copies(s1, l1s, p1_s, p1_r, plus1, minus1)

    def p2s1(t):
        s = lax.rem(t, 2)
        return first_copies(r1.at[s], q2, B2, l2f.at[s], l2d.at[s], p2_s.at[s], p2_r.at[s], plus2, minus2)

    def p2s2(t):
        s = lax.rem(t, 2)
        return second_copies(s2, l2s.at[s], p2_s.at[s], p2_r.at[s], plus2, minus2)

    def row0(t):
        return t * TT + c * HALF

    def rows_a(t, d):
        return pl.ds(pl.multiple_of(row0(t) + q1 * B1 + lax.rem(q2 + d + R, R) * B2, B2), B2)

    def rows_b(t, d):
        return pl.ds(pl.multiple_of(row0(t) + lax.rem(q1 + d + R, R) * B1, B1), B1)

    def same(rows, cols, ss, rs, dev):
        return rc(stage_ref.at[rows, cols], stage_ref.at[rows, cols], ss, rs, dev)

    def sl(t):
        return lax.rem(t, 4)

    def aga1(t):
        s, r = sl(t), rows_a(t, 0)
        return (rc(yrow, stage_ref.at[r, :], aga_s.at[s, 0], aga_r.at[s, 0], plus2),
                rc(yrow, stage_ref.at[r, :], aga_s.at[s, 1], aga_r.at[s, 1], minus2))

    def aga2(t):
        s = sl(t)
        return (same(rows_a(t, -1), DA, aga_s.at[s, 2], aga_r.at[s, 2], plus2),
                same(rows_a(t, 1), DB, aga_s.at[s, 3], aga_r.at[s, 3], minus2))

    def agb1(t):
        s, r = sl(t), rows_b(t, 0)
        return (same(r, pl.ds(0, D), agb_s.at[s, 0], agb_r.at[s, 0], plus1),
                same(r, pl.ds(0, D), agb_s.at[s, 1], agb_r.at[s, 1], minus1))

    def agb2(t):
        s = sl(t)
        return (same(rows_b(t, -1), DA, agb_s.at[s, 2], agb_r.at[s, 2], plus1),
                same(rows_b(t, 1), DB, agb_s.at[s, 3], agb_r.at[s, 3], minus1))

    def dd(t):
        s, r = sl(t), pl.ds(pl.multiple_of(row0(t), HALF), HALF)
        return same(r, pl.ds(0, D), dd_s.at[s], dd_r.at[s], mate)

    def yloc(t):
        return pltpu.make_async_copy(yrow, stage_ref.at[rows_a(t, 0), :], loc_sem.at[0])

    def xload(t):
        return pltpu.make_async_copy(x_ref.at[rows_a(t, 0), :], xrow, loc_sem.at[1])

    def start(cs):
        for cp in cs:
            cp.start()

    def wrecv(cs):
        for cp in cs:
            cp.wait_recv()

    def wsend(cs):
        for cp in cs:
            cp.wait_send()

    def comb(src, q, rows, lf, ld, sm, dst):
        sm[0] = src[blk(q, 1, rows), A] + lf[0]
        sm[1] = src[blk(q, -1, rows), B] + lf[1]
        dst[:, A] = src[blk(q, 0, rows), A] + ld[1]
        dst[:, B] = src[blk(q, 0, rows), B] + ld[0]

    def e1(t):
        wrecv(p1s1(t))
        wsend(p1s1(t))

        @pl.when(t >= 1)
        def _():
            wsend(p1s2(t - 1))
        comb(r0, q1, B1, l1f, l1d, s1, r1.at[lax.rem(t, 2)])
        start(p1s2(t))

    def e2(t):
        s = lax.rem(t, 2)
        wrecv(p1s2(t))
        r1[s, :, A] = r1[s, :, A] + l1s[0]
        r1[s, :, B] = r1[s, :, B] + l1s[1]
        start(p2s1(t))

    def e3(t):
        s = lax.rem(t, 2)
        wrecv(p2s1(t))
        wsend(p2s1(t))

        @pl.when(t >= 1)
        def _():
            wsend(p2s2(t - 1))
        comb(r1.at[s], q2, B2, l2f.at[s], l2d.at[s], s2, r2)
        start(p2s2(t))
        xload(t).start()

    def e4(t):
        s = lax.rem(t, 2)
        wrecv(p2s2(t))
        xload(t).wait()
        i = ids_ref[t // tps]
        r2[:, A] = r2[:, A] + l2s[s, 0]
        r2[:, B] = r2[:, B] + l2s[s, 1]
        lor = jnp.dot(r2[:, pl.ds(D, W - D)], bod_v[i], preferred_element_type=jnp.float32)
        y = xrow[...].astype(jnp.float32) + r2[:, pl.ds(0, D)].astype(jnp.float32) + scale * lor
        yrow[...] = y.astype(BF)
        yloc(t).start()
        start(aga1(t))

    def e5(t):
        yloc(t).wait()
        wsend(aga1(t))
        wrecv(aga1(t))
        start(aga2(t))

    def e6(t):
        wrecv(aga2(t))
        start(agb1(t))

    def e7(t):
        wrecv(agb1(t))
        start(agb2(t))

    def e8(t):
        wrecv(agb2(t))
        start((dd(t),))

    def e9(t):
        wrecv((dd(t),))
        wsend((dd(t),))
        wsend(agb2(t))
        wsend(agb1(t))
        wsend(aga2(t))

    F32 = jnp.float32

    def pa(t, hf):
        u = 2 * t + hf
        settle(t, hf, 0)
        xcopy(u).wait()

        @pl.when(u + 1 < 2 * NT)
        def _():
            xcopy(u + 1).start()
        i = ids_ref[t // tps]
        mids[...] = lax.dot_general(hbuf[hf], at_v[i], (((1,), (1,)), ((), ())), preferred_element_type=F32).astype(BF)

    def rope(z, rows):
        return z * cos_v[rows, :] + pltpu.roll(z, HEAD // 2, 1) * sin_v[rows, :]

    def pb(t, hf):
        settle(t, hf, 1)
        i = ids_ref[t // tps]
        pos = pl.ds(pl.multiple_of(lax.rem(t, tps) * TT + hf * HALF, HALF), HALF)
        z = jnp.dot(hbuf[hf], wqkv_v[...], preferred_element_type=F32)
        lqk = jnp.dot(mids[:, pl.ds(0, 2 * HEAD)], bqk_v[i], preferred_element_type=F32)
        lv = jnp.dot(mids[:, pl.ds(2 * HEAD, 2 * HEAD)], bv_v[i], preferred_element_type=F32)
        qbuf[...] = rope(z[:, :HEAD] + scale * lqk[:, :HEAD], pos).astype(BF)
        kbuf[pos, :] = rope(z[:, HEAD:2 * HEAD] + scale * lqk[:, HEAD:], pos).astype(BF)
        vbuf[pos, :] = (z[:, 2 * HEAD:] + scale * lv).astype(BF)

    def pc(t, hf):
        settle(t, hf, 2)
        i = ids_ref[t // tps]
        for n in range(FF // FB):
            cols = pl.ds(n * 2 * FB, 2 * FB)
            z = jnp.dot(hbuf[hf], wgu_v[:, cols], preferred_element_type=F32)
            z = z + scale * jnp.dot(mids[:, pl.ds(4 * HEAD, 2 * HEAD)], bgu_v[i, :, cols], preferred_element_type=F32)
            g = z[:, :FB]
            om[lax.rem(t, 2), hf, :, pl.ds(HEAD + n * FB, FB)] = (g * (1.0 / (1.0 + jnp.exp(-g))) * z[:, FB:]).astype(BF)

    def pd(t, hf):
        sc = lax.dot_general(qbuf[...], kbuf[...], (((1,), (1,)), ((), ())), preferred_element_type=F32) * (1.0 / math.sqrt(HEAD))
        row = lax.rem(t, tps) * TT + hf * HALF + lax.broadcasted_iota(jnp.int32, (HALF, KV), 0)
        col = lax.broadcasted_iota(jnp.int32, (HALF, KV), 1)
        sc = jnp.where(row >= col, sc, -1e30)
        e = jnp.exp(sc - jnp.max(sc, axis=-1, keepdims=True))
        p = (e / jnp.sum(e, axis=-1, keepdims=True)).astype(BF)
        om[lax.rem(t, 2), hf, :, pl.ds(0, HEAD)] = jnp.dot(p, vbuf[...], preferred_element_type=F32).astype(BF)

    def out_proj(t, half, dst, extra):
        i = ids_ref[t // tps]
        act = om[lax.rem(t, 2), half]
        last = jnp.dot(act, aod_v[i], preferred_element_type=F32)
        tail = pl.ds(D, W - D)
        dst[:, tail] = (last if extra is None else last + extra[:, tail].astype(F32)).astype(BF)
        NB = 512
        for n in range(D // NB):
            cols = pl.ds(n * NB, NB)
            acc = jnp.dot(act, wod_v[:, cols], preferred_element_type=F32)
            dst[:, cols] = (acc if extra is None else acc + extra[:, cols].astype(F32)).astype(BF)

    def pf(t):
        settle(t, 0, 3)

        @pl.when(t >= 1)
        def _():
            d2d(t - 1).wait_send()
        out_proj(t, 1 - c, psend, None)
        d2d(t).start()

    def pg(t):
        d2d(t).wait_recv()
        out_proj(t, c, r0, l0.at[lax.rem(t, 2)])
        start(p1s1(t))

    def guard(t, f, *a):
        @pl.when(jnp.logical_and(t >= 0, t < NT))
        def _():
            f(t, *a)

    def piece(ad, d, k, dev):
        ref = bod_v.at[ad, :, bcols(d)] if ad is not None else bod_v.at[:, :, bcols(d)]
        return rc(ref, ref, bg_s.at[k], bg_r.at[k], dev)

    def line(dev, k):
        return dev + (k - q2) * st2

    def g1():
        return (piece(None, idx, 0, plus2), piece(None, idx, 1, minus2))

    def g2():
        return (piece(0, minus2, 2, plus2), piece(1, plus2, 3, minus2))

    def g3():
        return tuple(piece(None, line(idx, k), 4 + k, plus1) for k in range(R)) + tuple(piece(None, line(idx, k), 4 + R + k, minus1) for k in range(R))

    def g4():
        return tuple(piece(0, line(minus1, k), 4 + 2 * R + k, plus1) for k in range(R)) + tuple(piece(1, line(plus1, k), 4 + 3 * R + k, minus1) for k in range(R))

    def g5():
        return tuple(piece(None, 2 * j + c, 4 + 4 * R + j, mate) for j in range(R * R))

    def b1():
        bown.wait()
        start(g1())

    def b2():
        wrecv(g1())
        start(g2())

    def b3():
        wrecv(g2())
        start(g3())

    def b4():
        wrecv(g3())
        start(g4())

    def b5():
        wrecv(g4())
        start(g5())

    def b6():
        for g in (g1, g2, g3, g4, g5):
            wsend(g())
        wrecv(g5())

    def at_step(it, k, f):
        @pl.when(it == k)
        def _():
            f()

    b1()

    def body(it, _):
        guard(it, pa, 0)
        guard(it, pb, 0)
        at_step(it, 0, b2)
        at_step(it, 1, b4)
        at_step(it, 3, b6)
        guard(it - 5, e7)
        guard(it - 4, e5)
        guard(it - 3, e4)
        guard(it - 2, e2)
        guard(it - 1, pg)
        guard(it, pc, 0)
        guard(it, pd, 0)
        guard(it, pa, 1)
        guard(it, pb, 1)
        at_step(it, 0, b3)
        at_step(it, 1, b5)
        guard(it - 1, e1)
        guard(it - 2, e3)
        guard(it - 4, e6)
        guard(it - 5, e8)
        guard(it - 6, e9)
        guard(it, pc, 1)
        guard(it, pd, 1)
        guard(it, pf)
        return 0
    lax.fori_loop(0, NT + 6, body, 0)
    last = NT - 1
    d2d(last).wait_send()
    wsend(p1s2(last))
    wsend(p2s2(last))


def fused(mesh, ids, x, h, at, wq, wk, wv, wg, wu, wo, wd, bqk, bv, bgu, aod, bown, cos, sin, scale, seq_len, TT):
    R = math.isqrt(mesh.shape["tensor"] // 2)
    T, D = x.shape
    HEAD, FF = wo.shape[0], wd.shape[0]
    W = D + aod.shape[-1]
    NT, HALF = T // TT, TT // 2
    B1 = HALF // R
    B2 = B1 // R
    WH = W // 2
    cfg = (R, NT, TT, W, D, HEAD, FF, scale, seq_len // TT)
    S = pltpu.SemaphoreType.DMA

    def V(*shape):
        return pltpu.VMEM(shape, BF)
    n_in = 17
    return pl.pallas_call(
        functools.partial(fused_kernel, cfg), name="block",
        out_shape=jax.ShapeDtypeStruct((T, D), BF),
        in_specs=[pl.BlockSpec(memory_space=pltpu.SMEM)] + [pl.BlockSpec(memory_space=pltpu.HBM)] * n_in,
        out_specs=pl.BlockSpec(memory_space=pltpu.HBM),
        scratch_shapes=[V(2, HALF, D), V(HALF, at.shape[1]), V(*at.shape), V(D, 3 * HEAD), V(D, 2 * FF), V(HEAD + FF, D),
                        V(*bqk.shape), V(*bv.shape), V(*bgu.shape), V(*aod.shape), V(*bown.shape[:2], D),
                        pltpu.VMEM(cos.shape, jnp.float32), pltpu.VMEM(sin.shape, jnp.float32), V(HALF, HEAD), V(seq_len, HEAD), V(seq_len, HEAD), V(2, 2, HALF, HEAD + FF),
                        V(HALF, W), V(2, HALF, W), V(HALF, W),
                        V(2, B1, WH), V(2, B1, WH), V(2, B1, WH), V(2, B1, WH), V(2, B1, W),
                        V(2, 2, B2, WH), V(2, 2, B2, WH), V(2, 2, B2, WH), V(2, B2, WH), V(B2, W),
                        V(B2, D), V(B2, D),
                        S((17,)), S((2,)), S, S((2,)), S((6,)), S((6,)), S((2, 6)), S((2, 6)), S((4, 4)), S((4, 4)), S((4, 4)), S((4, 4)), S((4,)), S((4,)), S((4 + 4 * R + R * R,)), S((4 + 4 * R + R * R,)), S((3,))],
        compiler_params=pltpu.CompilerParams(collective_id=0, has_side_effects=True, vmem_limit_bytes=67043328),
    )(ids, x, h, at, wq, wk, wv, wg, wu, wo, wd, bqk, bv, bgu, aod, bown, cos, sin)


def norm_kernel(x_ref, gain_ref, h_ref):
    rows_per = 16
    dim = x_ref.shape[1]

    def step(k, _):
        rows = pl.ds(pl.multiple_of(k * rows_per, rows_per), rows_per)
        xf = x_ref[rows, :].astype(jnp.float32)
        inv = lax.rsqrt(jnp.sum(xf * xf, axis=-1, keepdims=True) * (1.0 / dim) + EPS)
        h_ref[rows, :] = (xf * inv * gain_ref[...]).astype(BF)
        return 0
    lax.fori_loop(0, x_ref.shape[0] // rows_per, step, 0, unroll=4)


def norm(x, gain):
    T, D = x.shape
    rows = 256
    return pl.pallas_call(
        norm_kernel, name="norm", grid=(T // rows,),
        out_shape=jax.ShapeDtypeStruct((T, D), BF),
        in_specs=[pl.BlockSpec((rows, D), lambda i: (i, 0)), pl.BlockSpec((1, D), lambda i: (0, 0))],
        out_specs=pl.BlockSpec((rows, D), lambda i: (i, 0)),
        cost_estimate=pl.CostEstimate(flops=8000 * T * D // 1000 * 1000, bytes_accessed=4 * T * D, transcendentals=0),
    )(x, gain)


def solution(mesh):
    batch_spec = P('data', None, None)
    head_cols = P(None, 'tensor', None)
    head_rows = P('tensor', None, None)
    ff_cols = P(None, 'tensor')
    ff_rows = P('tensor', None)
    last_split = P(None, None, 'tensor')
    b_heads = P(None, None, 'tensor', None)
    a_heads = P(None, 'tensor', None, None)
    in_specs = (batch_spec, P('data'), P(None), head_cols, head_cols, head_cols, head_rows, ff_cols, ff_cols, ff_rows, last_split, b_heads, last_split, b_heads, last_split, b_heads, a_heads, last_split, last_split, last_split, last_split, last_split, head_cols, last_split)

    def local_layer(x_blk, adapter_ids, norm_gain, w_query, w_key, w_value, w_out, w_gate, w_up, w_down, a_query, b_query, a_key, b_key, a_value, b_value, a_out, b_out, a_gate, b_gate, a_up, b_up, a_down, b_down):
        seq_len = x_blk.shape[1]
        rank = a_out.shape[-1]
        scale = ALPHA / rank
        n_dev = mesh.shape['tensor']
        dim = x_blk.shape[2]
        n_ad = a_query.shape[0]
        zero_a = jnp.zeros_like(a_value)
        mine = jnp.concatenate([a_query, a_key, a_value, zero_a, a_gate, a_up], axis=2)
        mine = jnp.transpose(mine, (0, 2, 1)).reshape(n_ad * 3, -1, dim)
        a_all = lax.all_gather(mine, 'tensor', axis=1, tiled=True)
        a_all = a_all.reshape(n_ad, -1, dim)
        b_own = jnp.concatenate([b_out, b_down], axis=1)
        x_flat = x_blk.reshape(-1, dim)
        normed = norm(x_flat, norm_gain.reshape(1, dim))

        def weave(b_first, b_second):
            first = b_first.reshape(n_ad, n_dev, rank // n_dev, -1)
            second = b_second.reshape(n_ad, n_dev, rank // n_dev, -1)
            return first, second

        def pair(b_first, b_second):
            first, second = weave(b_first, b_second)
            zf, zs = jnp.zeros_like(first), jnp.zeros_like(second)
            rows = jnp.concatenate([jnp.concatenate([first, zs], axis=3), jnp.concatenate([zf, second], axis=3)], axis=2)
            return rows.reshape(n_ad, 2 * rank, -1)

        head = w_query.shape[-1]
        ff = w_gate.shape[1]
        tile = seq_len // 2
        fb = tile // 2
        bqk = pair(b_query, b_key)
        bv_first, _ = weave(b_value, b_value)
        bv = jnp.concatenate([bv_first, jnp.zeros_like(bv_first)], axis=2).reshape(n_ad, 2 * rank, -1)
        bgu = pair(b_gate, b_up).reshape(n_ad, 2 * rank, 2, ff // fb, fb)
        bgu = jnp.transpose(bgu, (0, 1, 3, 2, 4)).reshape(n_ad, 2 * rank, 2 * ff)
        ao = a_out.reshape(n_ad, head, rank)
        aod = jnp.concatenate([jnp.concatenate([ao, jnp.zeros_like(ao)], axis=2), jnp.concatenate([jnp.zeros_like(a_down), a_down], axis=2)], axis=1)
        half = head // 2
        inv_freq = ROPE_BASE ** (-jnp.arange(half, dtype=jnp.float32) / half)
        angles = jnp.arange(seq_len, dtype=jnp.float32)[:, None] * inv_freq[None, :]
        cos_t, sin_t = jnp.cos(angles), jnp.sin(angles)
        cos_t = jnp.concatenate([cos_t, cos_t], axis=1)
        sin_t = jnp.concatenate([-sin_t, sin_t], axis=1)
        out = fused(mesh, adapter_ids, x_flat, normed, a_all, w_query.reshape(dim, head), w_key.reshape(dim, head), w_value.reshape(dim, head),
                    w_gate, w_up, w_out.reshape(head, dim), w_down, bqk, bv, bgu, aod, b_own, cos_t, sin_t, scale, seq_len, tile)
        return out.reshape(x_blk.shape)

    return jax.shard_map(local_layer, mesh=mesh, in_specs=in_specs, out_specs=batch_spec, check_vma=False)
```

```python
import functools
import math

import jax
import jax.numpy as jnp
import numpy as np
from jax import lax
from jax.experimental import pallas as pl
from jax.experimental.pallas import tpu as pltpu
from jax.sharding import PartitionSpec as P

ALPHA = 16
EPS = 1e-5
ROPE_BASE = 10000.0
MESH = pl.DeviceIdType.MESH
BF = jnp.bfloat16

def fused_kernel(cfg, ids_ref, x_ref, gain_ref, aown_ref, wq_ref, wk_ref, wv_ref, wg_ref, wu_ref, wo_ref, wd_ref, bin_ref, ao_ref, ad_ref,
                 bown_ref, cos_ref, sin_ref, stage_ref,
                 xbuf, hbuf, mids, gain_v, at_v, wqkv_v, wgu_v, wod_v, bin_v, aod_v, bod_v, cos_v, sin_v, qbuf, kbuf, vbuf, om,
                 psend, l0, r0, l1f, l1d, l1s, s1, r1, l2f, l2d, l2s, s2, r2, xrow, yrow,
                 w_sem, x_sem, d2d_s, d2d_r, p1_s, p1_r, p2_s, p2_r, aga_s, aga_r, agb_s, agb_r, dd_s, dd_r, ag_s, ag_r, bg_s, bg_r, loc_sem):
    R, NT, TT, W, D, HEAD, FF, scale, tps = cfg
    HALF = TT // 2
    B1 = HALF // R
    B2 = B1 // R
    WH = W // 2
    DH = D // 2
    KV = tps * TT
    FB = HALF
    RANK = (W - D) // 2
    AR = aown_ref.shape[1]
    idx = lax.axis_index("tensor")
    c = lax.rem(idx, 2)
    xx = lax.rem(idx // 2, R)
    yy = idx // (2 * R)
    q1 = jnp.where(c == 0, xx, yy)
    q2 = jnp.where(c == 0, yy, xx)
    st1 = 2 + (2 * R - 2) * c
    st2 = 2 * R - (2 * R - 2) * c
    base1 = idx - q1 * st1
    base2 = idx - q2 * st2
    plus1 = base1 + lax.rem(q1 + 1, R) * st1
    minus1 = base1 + lax.rem(q1 + R - 1, R) * st1
    plus2 = base2 + lax.rem(q2 + 1, R) * st2
    minus2 = base2 + lax.rem(q2 + R - 1, R) * st2
    mate = idx + 1 - 2 * c
    peers = (mate, plus1, minus1, plus2, minus2)

    resident = (
        ((gain_ref, gain_v),),
        ((wq_ref, wqkv_v.at[:, pl.ds(0, HEAD)]), (wk_ref, wqkv_v.at[:, pl.ds(HEAD, HEAD)]), (wv_ref, wqkv_v.at[:, pl.ds(2 * HEAD, HEAD)]),
         (bin_ref, bin_v), (cos_ref, cos_v), (sin_ref, sin_v)),
        ((wg_ref.at[:, pl.ds(0, FB)], wgu_v.at[:, pl.ds(0, FB)]), (wu_ref.at[:, pl.ds(0, FB)], wgu_v.at[:, pl.ds(FB, FB)]),
         (wg_ref.at[:, pl.ds(FB, FB)], wgu_v.at[:, pl.ds(2 * FB, FB)]), (wu_ref.at[:, pl.ds(FB, FB)], wgu_v.at[:, pl.ds(3 * FB, FB)])),
        ((wo_ref, wod_v.at[pl.ds(0, HEAD), :]), (wd_ref, wod_v.at[pl.ds(HEAD, FF), :]), (ao_ref, aod_v.at[:, pl.ds(0, HEAD), pl.ds(0, RANK)]), (ad_ref, aod_v.at[:, pl.ds(HEAD, FF), pl.ds(RANK, RANK)])),
    )
    copies = []
    n_sem = 0
    for group in resident:
        row = []
        for src, dst in group:
            row.append(pltpu.make_async_copy(src, dst, w_sem.at[n_sem]))
            n_sem += 1
        copies.append(row)

    def xcopy(u):
        rows = pl.ds(pl.multiple_of(u * HALF, HALF), HALF)
        s = lax.rem(u, 2)
        return pltpu.make_async_copy(x_ref.at[rows, :], xbuf.at[s], x_sem.at[s])

    CB = bown_ref.shape[-1]

    def bcols(d):
        return pl.ds(pl.multiple_of(d * CB, CB), CB)

    bown = pltpu.make_async_copy(bown_ref, bod_v.at[:, :, bcols(idx)], loc_sem.at[2])
    def arows(d):
        return pl.ds(pl.multiple_of(d * AR, AR), AR)

    aown = pltpu.make_async_copy(aown_ref, at_v.at[:, arows(idx), :], loc_sem.at[3])
    aown.start()
    xcopy(0).start()
    aod_v[...] = jnp.zeros_like(aod_v)
    for row in copies:
        for cp in row:
            cp.start()

    bown.start()

    bar = pltpu.get_barrier_semaphore()
    for p in peers:
        pl.semaphore_signal(bar, inc=1, device_id={"tensor": p}, device_id_type=MESH)
    pl.semaphore_wait(bar, len(peers))
    vbuf[...] = jnp.zeros_like(vbuf)
    kbuf[...] = jnp.zeros_like(kbuf)

    def settle(t, hf, k):
        if isinstance(t, int):
            for cp in copies[k]:
                cp.wait()
        elif hf == 0 and k > 0:
            @pl.when(t == 0)
            def _():
                for cp in copies[k]:
                    cp.wait()

    def rc(src, dst, ss, rs, dev):
        return pltpu.make_async_remote_copy(src_ref=src, dst_ref=dst, send_sem=ss, recv_sem=rs, device_id={"tensor": dev}, device_id_type=MESH)

    def blk(q, d, rows):
        return pl.ds(pl.multiple_of(lax.rem(q + d + R, R) * rows, rows), rows)

    A, B = pl.ds(0, WH), pl.ds(WH, WH)
    DA, DB = pl.ds(0, DH), pl.ds(DH, DH)

    def d2d(t):
        s = lax.rem(t, 2)
        return tuple(rc(psend.at[:, cols], l0.at[s, :, cols], d2d_s.at[k], d2d_r.at[s, k], mate) for k, cols in enumerate((A, B)))

    def first_copies(src, q, rows, lf, ld, ss, rs, plus, minus):
        return (rc(src.at[blk(q, 2, rows), A], lf.at[0], ss.at[0], rs.at[0], plus),
                rc(src.at[blk(q, 2, rows), B], lf.at[1], ss.at[1], rs.at[1], minus),
                rc(src.at[blk(q, 1, rows), B], ld.at[0], ss.at[2], rs.at[2], plus),
                rc(src.at[blk(q, -1, rows), A], ld.at[1], ss.at[3], rs.at[3], minus))

    def second_copies(sm, ls, ss, rs, plus, minus):
        return (rc(sm.at[0], ls.at[0], ss.at[4], rs.at[4], plus),
                rc(sm.at[1], ls.at[1], ss.at[5], rs.at[5], minus))

    def p1s1(t):
        return first_copies(r0, q1, B1, l1f, l1d, p1_s, p1_r, plus1, minus1)

    def p1s2(t):
        return second_copies(s1, l1s, p1_s, p1_r, plus1, minus1)

    def p2s1(t):
        s = lax.rem(t, 2)
        return first_copies(r1.at[s], q2, B2, l2f.at[s], l2d.at[s], p2_s.at[s], p2_r.at[s], plus2, minus2)

    def p2s2(t):
        s = lax.rem(t, 2)
        return second_copies(s2, l2s.at[s], p2_s.at[s], p2_r.at[s], plus2, minus2)

    def row0(t):
        return t * TT + c * HALF

    def rows_a(t, d):
        return pl.ds(pl.multiple_of(row0(t) + q1 * B1 + lax.rem(q2 + d + R, R) * B2, B2), B2)

    def rows_b(t, d):
        return pl.ds(pl.multiple_of(row0(t) + lax.rem(q1 + d + R, R) * B1, B1), B1)

    def same(rows, cols, ss, rs, dev):
        return rc(stage_ref.at[rows, cols], stage_ref.at[rows, cols], ss, rs, dev)

    def sl(t):
        return lax.rem(t, 4)

    def aga1(t):
        s, r = sl(t), rows_a(t, 0)
        return (rc(yrow, stage_ref.at[r, :], aga_s.at[s, 0], aga_r.at[s, 0], plus2),
                rc(yrow, stage_ref.at[r, :], aga_s.at[s, 1], aga_r.at[s, 1], minus2))

    def aga2(t):
        s = sl(t)
        return (same(rows_a(t, -1), DA, aga_s.at[s, 2], aga_r.at[s, 2], plus2),
                same(rows_a(t, 1), DB, aga_s.at[s, 3], aga_r.at[s, 3], minus2))

    def agb1(t):
        s, r = sl(t), rows_b(t, 0)
        return (same(r, pl.ds(0, D), agb_s.at[s, 0], agb_r.at[s, 0], plus1),
                same(r, pl.ds(0, D), agb_s.at[s, 1], agb_r.at[s, 1], minus1))

    def agb2(t):
        s = sl(t)
        return (same(rows_b(t, -1), DA, agb_s.at[s, 2], agb_r.at[s, 2], plus1),
                same(rows_b(t, 1), DB, agb_s.at[s, 3], agb_r.at[s, 3], minus1))

    def dd(t):
        s, r = sl(t), pl.ds(pl.multiple_of(row0(t), HALF), HALF)
        return same(r, pl.ds(0, D), dd_s.at[s], dd_r.at[s], mate)

    def yloc(t):
        return pltpu.make_async_copy(yrow, stage_ref.at[rows_a(t, 0), :], loc_sem.at[0])

    def xload(t):
        return pltpu.make_async_copy(x_ref.at[rows_a(t, 0), :], xrow, loc_sem.at[1])

    def start(cs):
        for cp in cs:
            cp.start()

    def wrecv(cs):
        for cp in cs:
            cp.wait_recv()

    def wsend(cs):
        for cp in cs:
            cp.wait_send()

    def comb(src, q, rows, lf, ld, sm, dst):
        sm[0] = src[blk(q, 1, rows), A] + lf[0]
        sm[1] = src[blk(q, -1, rows), B] + lf[1]
        dst[:, A] = src[blk(q, 0, rows), A] + ld[1]
        dst[:, B] = src[blk(q, 0, rows), B] + ld[0]

    def e1(t):
        wrecv(p1s1(t))
        wsend(p1s1(t))

        @pl.when(t >= 1)
        def _():
            wsend(p1s2(t - 1))
        comb(r0, q1, B1, l1f, l1d, s1, r1.at[lax.rem(t, 2)])
        start(p1s2(t))

    def e2(t):
        s = lax.rem(t, 2)
        wrecv(p1s2(t))
        r1[s, :, A] = r1[s, :, A] + l1s[0]
        r1[s, :, B] = r1[s, :, B] + l1s[1]
        start(p2s1(t))

    def e3(t):
        s = lax.rem(t, 2)
        wrecv(p2s1(t))
        wsend(p2s1(t))

        @pl.when(t >= 1)
        def _():
            wsend(p2s2(t - 1))
        comb(r1.at[s], q2, B2, l2f.at[s], l2d.at[s], s2, r2)
        start(p2s2(t))
        xload(t).start()

    def e4(t):
        s = lax.rem(t, 2)
        wrecv(p2s2(t))
        xload(t).wait()
        i = ids_ref[t // tps]
        r2[:, A] = r2[:, A] + l2s[s, 0]
        r2[:, B] = r2[:, B] + l2s[s, 1]
        lor = jnp.dot(r2[:, pl.ds(D, W - D)], bod_v[i], preferred_element_type=jnp.float32)
        y = xrow[...].astype(jnp.float32) + r2[:, pl.ds(0, D)].astype(jnp.float32) + scale * lor
        yrow[...] = y.astype(BF)
        yloc(t).start()
        start(aga1(t))

    def e5(t):
        yloc(t).wait()
        wsend(aga1(t))
        wrecv(aga1(t))
        start(aga2(t))

    def e6(t):
        wrecv(aga2(t))
        start(agb1(t))

    def e7(t):
        wrecv(agb1(t))
        start(agb2(t))

    def e8(t):
        wrecv(agb2(t))
        wsend(agb1(t))
        wsend(aga2(t))
        start((dd(t),))

    def e9(t):
        wrecv((dd(t),))
        wsend((dd(t),))
        wsend(agb2(t))

    F32 = jnp.float32

    def pn(t, hf):
        u = 2 * t + hf
        settle(t, hf, 0)
        xcopy(u).wait()

        @pl.when(u + 1 < 2 * NT)
        def _():
            xcopy(u + 1).start()
        s = lax.rem(u, 2)
        RB = 16

        def step(k, _):
            rows = pl.ds(pl.multiple_of(k * RB, RB), RB)
            xf = xbuf[s, rows, :].astype(F32)
            inv = lax.rsqrt(jnp.sum(xf * xf, axis=-1, keepdims=True) * (1.0 / D) + EPS)
            hbuf[rows, :] = (xf * inv * gain_v[...]).astype(BF)
            return 0
        lax.fori_loop(0, HALF // RB, step, 0, unroll=8)

    def nt(a, b):
        return lax.dot_general(a, b, (((1,), (1,)), ((), ())), preferred_element_type=F32)

    def pm(t, hf):
        i = ids_ref[t // tps]
        n = at_v.shape[1]
        both = at_v[pl.ds(2 * i, 2)].reshape(2 * n, D)
        mids[:, pl.ds(0, 2 * n)] = nt(hbuf[...], both).astype(BF)
        mids[:, pl.ds(2 * n, n)] = nt(hbuf[...], at_v[at_v.shape[0] - 1]).astype(BF)

    def rope(z, rows):
        return z * cos_v[rows, :] + pltpu.roll(z, HEAD // 2, 1) * sin_v[rows, :]

    def pb(t, hf):
        settle(t, hf, 1)
        i = ids_ref[t // tps]
        pos = pl.ds(pl.multiple_of(lax.rem(t, tps) * TT + hf * HALF, HALF), HALF)
        z = jnp.dot(hbuf[...], wqkv_v[...], preferred_element_type=F32)
        n = at_v.shape[1]
        lqk = jnp.dot(mids[:, pl.ds(0, n)], bin_v[i, :, pl.ds(0, 2 * HEAD)], preferred_element_type=F32)
        lv = jnp.dot(mids[:, pl.ds(2 * n, n)], bin_v[i, :, pl.ds(2 * HEAD, HEAD)], preferred_element_type=F32)
        qbuf[...] = rope(z[:, :HEAD] + scale * lqk[:, :HEAD], pos).astype(BF)
        kbuf[pos, :] = rope(z[:, HEAD:2 * HEAD] + scale * lqk[:, HEAD:], pos).astype(BF)
        vbuf[pos, :] = (z[:, 2 * HEAD:] + scale * lv).astype(BF)

    def pc(t, hf):
        settle(t, hf, 2)
        i = ids_ref[t // tps]
        for n in range(FF // FB):
            cols = pl.ds(n * 2 * FB, 2 * FB)
            z = jnp.dot(hbuf[...], wgu_v[:, cols], preferred_element_type=F32)
            z = z + scale * jnp.dot(mids[:, pl.ds(at_v.shape[1], at_v.shape[1])], bin_v[i, :, pl.ds(3 * HEAD + n * 2 * FB, 2 * FB)], preferred_element_type=F32)
            g = z[:, :FB]
            om[lax.rem(t, 2), hf, :, pl.ds(HEAD + n * FB, FB)] = (g * (1.0 / (1.0 + jnp.exp(-g))) * z[:, FB:]).astype(BF)

    def pd(t, hf):
        sc = lax.dot_general(qbuf[...], kbuf[...], (((1,), (1,)), ((), ())), preferred_element_type=F32) * (1.0 / math.sqrt(HEAD))
        row = lax.rem(t, tps) * TT + hf * HALF + lax.broadcasted_iota(jnp.int32, (HALF, KV), 0)
        col = lax.broadcasted_iota(jnp.int32, (HALF, KV), 1)
        sc = jnp.where(row >= col, sc, -1e30)
        e = jnp.exp(sc - jnp.max(sc, axis=-1, keepdims=True))
        p = (e / jnp.sum(e, axis=-1, keepdims=True)).astype(BF)
        om[lax.rem(t, 2), hf, :, pl.ds(0, HEAD)] = jnp.dot(p, vbuf[...], preferred_element_type=F32).astype(BF)

    def out_proj(t, half, dst, extra, hooks):
        i = ids_ref[t // tps]
        act = om[lax.rem(t, 2), half]
        NB = 512
        for n in range(D // NB + 1):
            cols = pl.ds(n * NB, min(NB, W - n * NB))
            if n in hooks:
                hooks[n]()
            w = wod_v[:, cols] if n < D // NB else aod_v[i]
            acc = jnp.dot(act, w, preferred_element_type=F32)
            dst[:, cols] = (acc if extra is None else acc + extra[:, cols].astype(F32)).astype(BF)

    def pf(t):
        settle(t, 0, 3)

        @pl.when(t >= 1)
        def _():
            wsend(d2d(t - 1))
        out_proj(t, 1 - c, psend, None, {5: lambda: d2d(t)[0].start()})
        d2d(t)[1].start()

    def pg(t):
        out_proj(t, c, r0, l0.at[lax.rem(t, 2)], {0: lambda: d2d(t)[0].wait_recv(), 4: lambda: d2d(t)[1].wait_recv(),
                                                 5: lambda: start(p1s1(t)[0::3])})
        start(p1s1(t)[1:3])

    def guard(t, f, *a):
        @pl.when(jnp.logical_and(t >= 0, t < NT))
        def _():
            f(t, *a)

    def piece(ad, d, k, dev):
        ref = bod_v.at[ad, :, bcols(d)] if ad is not None else bod_v.at[:, :, bcols(d)]
        return rc(ref, ref, bg_s.at[k], bg_r.at[k], dev)

    def line(dev, k):
        return dev + (k - q2) * st2

    def g1():
        return (piece(None, idx, 0, plus2), piece(None, idx, 1, minus2))

    def g2():
        return (piece(0, minus2, 2, plus2), piece(1, plus2, 3, minus2))

    def g3():
        return tuple(piece(None, line(idx, k), 4 + k, plus1) for k in range(R)) + tuple(piece(None, line(idx, k), 4 + R + k, minus1) for k in range(R))

    def g4():
        return tuple(piece(0, line(minus1, k), 4 + 2 * R + k, plus1) for k in range(R)) + tuple(piece(1, line(plus1, k), 4 + 3 * R + k, minus1) for k in range(R))

    def g5():
        return tuple(piece(None, 2 * j + c, 4 + 4 * R + j, mate) for j in range(R * R))

    def b1():
        bown.wait()
        start(g1())

    def b2():
        wrecv(g1())
        start(g2())

    def b3():
        wrecv(g2())
        start(g3())

    def b4():
        wrecv(g3())
        start(g4())

    def b5():
        wrecv(g4())
        start(g5())

    def b6():
        for g in (g1, g2, g3, g4, g5):
            wsend(g())
        wrecv(g5())

    def at_step(it, k, f):
        @pl.when(it == k)
        def _():
            f()

    def ln(dev, r):
        return dev - q2 * st2 + lax.rem(q2 + r + R, R) * st2

    def arow(d, k, dev, cols):
        ref = at_v.at[:, arows(d), cols]
        return rc(ref, ref, ag_s.at[k], ag_r.at[k], dev)

    full = pl.ds(0, D)
    opp1 = base1 + lax.rem(q1 + 2, R) * st1
    lines = (idx, minus1, plus1, opp1)

    def a1():
        return (arow(idx, 0, plus2, full), arow(idx, 1, minus2, full))

    def a2():
        return (arow(minus2, 2, plus2, DA), arow(plus2, 3, minus2, DB))

    def ab(r):
        return (arow(ln(idx, r), 4 + r % R, plus1, full), arow(ln(idx, r), 4 + R + r % R, minus1, full))

    def af(r):
        return (arow(ln(minus1, r), 4 + 2 * R + r % R, plus1, DA), arow(ln(plus1, r), 4 + 3 * R + r % R, minus1, DB))

    def am(j, r):
        return (arow(ln(lines[j], r), 4 + 4 * R + R * j + r % R, mate, full),)

    def gather_a():
        aown.wait()
        start(a1())
        start(ab(0))
        start(am(0, 0))
        pn(0, 0)
        wrecv(a1())
        start(a2())
        for r in (-1, 1):
            start(ab(r))
            start(am(0, r))
        wrecv(a2())
        start(ab(2))
        start(am(0, 2))
        for r in (0, -1, 1, 2):
            wrecv(ab(r))
            start(af(r))
            start(am(1, r))
            start(am(2, r))
        for r in (0, -1, 1, 2):
            wrecv(af(r))
            start(am(3, r))
        for j in range(4):
            for r in (0, -1, 1, 2):
                wrecv(am(j, r))
        wsend(a1())
        wsend(a2())
        for r in (0, -1, 1, 2):
            wsend(ab(r))
            wsend(af(r))
            for j in range(4):
                wsend(am(j, r))

    gather_a()
    b1()

    def body(it, _):
        at_step(it, 3, b6)
        @pl.when(jnp.logical_and(it >= 1, it < NT))
        def _():
            pn(it, 0)
        guard(it - 3, e4)
        guard(it, pm, 0)
        guard(it - 2, e2)
        guard(it - 1, pg)
        guard(it, pb, 0)
        at_step(it, 0, b2)
        at_step(it, 1, b4)
        guard(it, pc, 0)
        guard(it - 5, e7)
        guard(it, pd, 0)
        guard(it, pn, 1)
        guard(it, pm, 1)
        guard(it - 3, e5)
        guard(it - 2, e3)
        guard(it, pb, 1)
        guard(it - 1, e1)
        at_step(it, 0, b3)
        at_step(it, 1, b5)
        guard(it, pc, 1)
        guard(it - 6, e8)
        guard(it, pd, 1)
        guard(it - 3, e6)
        guard(it, pf)
        guard(it - 7, e9)
        return 0
    lax.fori_loop(0, NT + 7, body, 0)
    last = NT - 1
    wsend(d2d(last))
    wsend(p1s2(last))
    wsend(p2s2(last))


def fused(mesh, ids, x, gain, aown, wq, wk, wv, wg, wu, wo, wd, b_in, ao, ad, bown, cos, sin, scale, seq_len, TT):
    R = math.isqrt(mesh.shape["tensor"] // 2)
    T, D = x.shape
    HEAD, FF = wo.shape[0], wd.shape[0]
    W = D + 2 * ao.shape[-1]
    NT, HALF = T // TT, TT // 2
    B1 = HALF // R
    B2 = B1 // R
    WH = W // 2
    cfg = (R, NT, TT, W, D, HEAD, FF, scale, seq_len // TT)
    S = pltpu.SemaphoreType.DMA

    def V(*shape):
        return pltpu.VMEM(shape, BF)
    n_in = 16
    rows_a = aown.shape[1] * mesh.shape["tensor"]
    return pl.pallas_call(
        functools.partial(fused_kernel, cfg), name="block",
        out_shape=jax.ShapeDtypeStruct((T, D), BF),
        in_specs=[pl.BlockSpec(memory_space=pltpu.SMEM)] + [pl.BlockSpec(memory_space=pltpu.HBM)] * n_in,
        out_specs=pl.BlockSpec(memory_space=pltpu.HBM),
        scratch_shapes=[V(2, HALF, D), V(HALF, D), V(HALF, 3 * rows_a), pltpu.VMEM(gain.shape, jnp.float32), V(aown.shape[0], rows_a, D), V(D, 3 * HEAD), V(D, 2 * FF), V(HEAD + FF, D),
                        V(*b_in.shape), V(ao.shape[0], HEAD + FF, W - D), V(*bown.shape[:2], D),
                        pltpu.VMEM(cos.shape, jnp.float32), pltpu.VMEM(sin.shape, jnp.float32), V(HALF, HEAD), V(seq_len, HEAD), V(seq_len, HEAD), V(2, 2, HALF, HEAD + FF),
                        V(HALF, W), V(2, HALF, W), V(HALF, W),
                        V(2, B1, WH), V(2, B1, WH), V(2, B1, WH), V(2, B1, WH), V(2, B1, W),
                        V(2, 2, B2, WH), V(2, 2, B2, WH), V(2, 2, B2, WH), V(2, B2, WH), V(B2, W),
                        V(B2, D), V(B2, D),
                        S((15,)), S((2,)), S((2,)), S((2, 2)), S((6,)), S((6,)), S((2, 6)), S((2, 6)), S((4, 4)), S((4, 4)), S((4, 4)), S((4, 4)), S((4,)), S((4,)), S((4 + 8 * R,)), S((4 + 8 * R,)), S((4 + 4 * R + R * R,)), S((4 + 4 * R + R * R,)), S((4,))],
        compiler_params=pltpu.CompilerParams(collective_id=0, has_side_effects=True, vmem_limit_bytes=67043328),
    )(ids, x, gain, aown, wq, wk, wv, wg, wu, wo, wd, b_in, ao, ad, bown, cos, sin)


def solution(mesh):
    batch_spec = P('data', None, None)
    head_cols = P(None, 'tensor', None)
    head_rows = P('tensor', None, None)
    ff_cols = P(None, 'tensor')
    ff_rows = P('tensor', None)
    last_split = P(None, None, 'tensor')
    b_heads = P(None, None, 'tensor', None)
    a_heads = P(None, 'tensor', None, None)
    in_specs = (batch_spec, P('data'), P(None), head_cols, head_cols, head_cols, head_rows, ff_cols, ff_cols, ff_rows, last_split, b_heads, last_split, b_heads, last_split, b_heads, a_heads, last_split, last_split, last_split, last_split, last_split, head_cols, last_split)

    def local_layer(x_blk, adapter_ids, norm_gain, w_query, w_key, w_value, w_out, w_gate, w_up, w_down, a_query, b_query, a_key, b_key, a_value, b_value, a_out, b_out, a_gate, b_gate, a_up, b_up, a_down, b_down):
        seq_len = x_blk.shape[1]
        rank = a_out.shape[-1]
        scale = ALPHA / rank
        n_dev = mesh.shape['tensor']
        dim = x_blk.shape[2]
        n_ad = a_query.shape[0]
        zero_a = jnp.zeros_like(a_value)
        part = rank // n_dev
        cols = [st[i] for i in range(n_ad) for st in (a_query, a_key, a_gate, a_up)] + [a_value[i] for i in range(n_ad)]
        mine = jnp.transpose(jnp.concatenate(cols, axis=1)).reshape(2 * n_ad + 1, 2 * part, dim)
        b_own = jnp.concatenate([b_out, b_down], axis=1)
        head = w_query.shape[-1]
        ff = w_gate.shape[1]
        tile = seq_len // 2
        fb = tile // 2

        def rows(stack):
            return stack.reshape(n_ad, n_dev, part, -1)

        bq, bk, bvv, bg, bu = (rows(b) for b in (b_query, b_key, b_value, b_gate, b_up))
        zq, zg = jnp.zeros_like(bq), jnp.zeros_like(bg[..., :fb])
        which = jnp.arange(n_ad).reshape(n_ad, 1, 1, 1)
        top, low = [bq, zq, jnp.where(which == 0, bvv, zq)], [zq, bk, jnp.where(which == 1, bvv, zq)]
        for n in range(ff // fb):
            top += [bg[..., n * fb:(n + 1) * fb], zg]
            low += [zg, bu[..., n * fb:(n + 1) * fb]]
        b_in = jnp.concatenate([jnp.concatenate(top, axis=3), jnp.concatenate(low, axis=3)], axis=2).reshape(n_ad, 2 * rank, -1)
        half = head // 2
        inv_freq = np.float32(ROPE_BASE) ** (-np.arange(half, dtype=np.float32) / np.float32(half))
        angles = np.arange(seq_len, dtype=np.float32)[:, None] * inv_freq[None, :]
        cos_t, sin_t = np.cos(angles), np.sin(angles)
        cos_t = jnp.asarray(np.concatenate([cos_t, cos_t], axis=1))
        sin_t = jnp.asarray(np.concatenate([-sin_t, sin_t], axis=1))
        out = fused(mesh, adapter_ids, x_blk.reshape(-1, dim), norm_gain.reshape(1, dim), mine, w_query.reshape(dim, head), w_key.reshape(dim, head), w_value.reshape(dim, head),
                    w_gate, w_up, w_out.reshape(head, dim), w_down, b_in, a_out.reshape(n_ad, head, rank), a_down, b_own, cos_t, sin_t, scale, seq_len, tile)
        return out.reshape(x_blk.shape)

    return jax.shard_map(local_layer, mesh=mesh, in_specs=in_specs, out_specs=batch_spec, check_vma=False)
```

```python
import functools
import math

import jax
import jax.numpy as jnp
import numpy as np
from jax import lax
from jax.experimental import pallas as pl
from jax.experimental.pallas import tpu as pltpu
from jax.sharding import PartitionSpec as P

ALPHA = 16
EPS = 1e-5
ROPE_BASE = 10000.0
MESH = pl.DeviceIdType.MESH
BF = jnp.bfloat16

def fused_kernel(cfg, ids_ref, x_ref, gain_ref, aown_ref, avown_ref, wq_ref, wk_ref, wv_ref, wg_ref, wu_ref, wo_ref, wd_ref, bq_ref, bk_ref, bv_ref, bg_ref, bu_ref, ao_ref, ad_ref,
                 bo_ref, bd_ref, cos_ref, sin_ref, stage_ref,
                 xbuf, hbuf, mids, gain_v, at_v, wqkv_v, wgu_v, wod_v, bst_v, bin_v, aod_v, bod_v, cos_v, sin_v, qbuf, kbuf, vbuf, om,
                 psend, l0, r0, l1f, l1d, l1s, s1, r1, l2f, l2d, l2s, s2, r2, xrow, yrow,
                 w_sem, x_sem, d2d_s, d2d_r, p1_s, p1_r, p2_s, p2_r, aga_s, aga_r, agb_s, agb_r, dd_s, dd_r, ag_s, ag_r, bg_s, bg_r, loc_sem):
    R, NT, TT, W, D, HEAD, FF, scale, tps = cfg
    HALF = TT // 2
    B1 = HALF // R
    B2 = B1 // R
    WH = W // 2
    DH = D // 2
    KV = tps * TT
    FB = HALF
    RANK = (W - D) // 2
    AR = aown_ref.shape[1]
    idx = lax.axis_index("tensor")
    c = lax.rem(idx, 2)
    xx = lax.rem(idx // 2, R)
    yy = idx // (2 * R)
    q1 = jnp.where(c == 0, xx, yy)
    q2 = jnp.where(c == 0, yy, xx)
    st1 = 2 + (2 * R - 2) * c
    st2 = 2 * R - (2 * R - 2) * c
    base1 = idx - q1 * st1
    base2 = idx - q2 * st2
    plus1 = base1 + lax.rem(q1 + 1, R) * st1
    minus1 = base1 + lax.rem(q1 + R - 1, R) * st1
    plus2 = base2 + lax.rem(q2 + 1, R) * st2
    minus2 = base2 + lax.rem(q2 + R - 1, R) * st2
    mate = idx + 1 - 2 * c
    peers = (mate, plus1, minus1, plus2, minus2)

    resident = (
        ((gain_ref, gain_v),),
        ((wq_ref, wqkv_v.at[:, pl.ds(0, HEAD)]), (wk_ref, wqkv_v.at[:, pl.ds(HEAD, HEAD)]), (wv_ref, wqkv_v.at[:, pl.ds(2 * HEAD, HEAD)]),
         (cos_ref, cos_v), (sin_ref, sin_v)),
        ((wg_ref.at[:, pl.ds(0, FB)], wgu_v.at[:, pl.ds(0, FB)]), (wu_ref.at[:, pl.ds(0, FB)], wgu_v.at[:, pl.ds(FB, FB)]),
         (wg_ref.at[:, pl.ds(FB, FB)], wgu_v.at[:, pl.ds(2 * FB, FB)]), (wu_ref.at[:, pl.ds(FB, FB)], wgu_v.at[:, pl.ds(3 * FB, FB)])),
        ((wo_ref, wod_v.at[pl.ds(0, HEAD), :]), (wd_ref, wod_v.at[pl.ds(HEAD, FF), :]), (ao_ref, aod_v.at[:, pl.ds(0, HEAD), pl.ds(0, RANK)]), (ad_ref, aod_v.at[:, pl.ds(HEAD, FF), pl.ds(RANK, RANK)])),
    )
    copies = []
    n_sem = 0
    for group in resident:
        row = []
        for src, dst in group:
            row.append(pltpu.make_async_copy(src, dst, w_sem.at[n_sem]))
            n_sem += 1
        copies.append(row)

    def xcopy(u):
        rows = pl.ds(pl.multiple_of(u * HALF, HALF), HALF)
        s = lax.rem(u, 2)
        return pltpu.make_async_copy(x_ref.at[rows, :], xbuf.at[s], x_sem.at[s])

    CB = bo_ref.shape[-1]

    def bcols(d):
        return pl.ds(pl.multiple_of(d * CB, CB), CB)

    bown = tuple(pltpu.make_async_copy(ref, bod_v.at[:, pl.ds(k * RANK, RANK), bcols(idx)], loc_sem.at[2 + k]) for k, ref in enumerate((bo_ref, bd_ref)))
    def arows(d):
        return pl.ds(pl.multiple_of(d * AR, AR), AR)

    n_qk = aown_ref.shape[0]
    aown = (pltpu.make_async_copy(aown_ref, at_v.at[pl.ds(0, n_qk), arows(idx), :], loc_sem.at[4]),
            pltpu.make_async_copy(avown_ref, at_v.at[pl.ds(n_qk, 1), arows(idx), :], loc_sem.at[5]))
    for cp in aown:
        cp.start()
    bcol = [(bq_ref, 0, HEAD, 0, 0), (bk_ref, HEAD, HEAD, 0, 1), (bv_ref, 2 * HEAD, HEAD, 0, 2)]
    for n in range(FF // FB):
        bcol += [(bg_ref, 3 * HEAD + 2 * n * FB, FB, n * FB, 0), (bu_ref, 3 * HEAD + (2 * n + 1) * FB, FB, n * FB, 1)]
    bload = [pltpu.make_async_copy(ref.at[:, :, pl.ds(at, width)], bst_v.at[:, :, pl.ds(col, width)], loc_sem.at[6 + k])
             for k, (ref, col, width, at, _) in enumerate(bcol)]
    for cp in bload:
        cp.start()
    xcopy(0).start()
    aod_v[...] = jnp.zeros_like(aod_v)
    for row in copies:
        for cp in row:
            cp.start()

    for cp in bown:
        cp.start()

    bar = pltpu.get_barrier_semaphore()
    for p in peers:
        pl.semaphore_signal(bar, inc=1, device_id={"tensor": p}, device_id_type=MESH)
    pl.semaphore_wait(bar, len(peers))
    vbuf[...] = jnp.zeros_like(vbuf)
    kbuf[...] = jnp.zeros_like(kbuf)

    def settle(t, hf, k):
        if isinstance(t, int):
            for cp in copies[k]:
                cp.wait()
        elif hf == 0 and k > 0:
            @pl.when(t == 0)
            def _():
                for cp in copies[k]:
                    cp.wait()

    def rc(src, dst, ss, rs, dev):
        return pltpu.make_async_remote_copy(src_ref=src, dst_ref=dst, send_sem=ss, recv_sem=rs, device_id={"tensor": dev}, device_id_type=MESH)

    def blk(q, d, rows):
        return pl.ds(pl.multiple_of(lax.rem(q + d + R, R) * rows, rows), rows)

    A, B = pl.ds(0, WH), pl.ds(WH, WH)
    DA, DB = pl.ds(0, DH), pl.ds(DH, DH)

    def d2d(t):
        s = lax.rem(t, 2)
        return tuple(rc(psend.at[:, cols], l0.at[s, :, cols], d2d_s.at[k], d2d_r.at[s, k], mate) for k, cols in enumerate((A, B)))

    def first_copies(src, q, rows, lf, ld, ss, rs, plus, minus):
        return (rc(src.at[blk(q, 2, rows), A], lf.at[0], ss.at[0], rs.at[0], plus),
                rc(src.at[blk(q, 2, rows), B], lf.at[1], ss.at[1], rs.at[1], minus),
                rc(src.at[blk(q, 1, rows), B], ld.at[0], ss.at[2], rs.at[2], plus),
                rc(src.at[blk(q, -1, rows), A], ld.at[1], ss.at[3], rs.at[3], minus))

    def second_copies(sm, ls, ss, rs, plus, minus):
        return (rc(sm.at[0], ls.at[0], ss.at[4], rs.at[4], plus),
                rc(sm.at[1], ls.at[1], ss.at[5], rs.at[5], minus))

    def p1s1(t):
        return first_copies(r0, q1, B1, l1f, l1d, p1_s, p1_r, plus1, minus1)

    def p1s2(t):
        return second_copies(s1, l1s, p1_s, p1_r, plus1, minus1)

    def p2s1(t):
        s = lax.rem(t, 2)
        return first_copies(r1.at[s], q2, B2, l2f.at[s], l2d.at[s], p2_s.at[s], p2_r.at[s], plus2, minus2)

    def p2s2(t):
        s = lax.rem(t, 2)
        return second_copies(s2, l2s.at[s], p2_s.at[s], p2_r.at[s], plus2, minus2)

    def row0(t):
        return t * TT + c * HALF

    def rows_a(t, d):
        return pl.ds(pl.multiple_of(row0(t) + q1 * B1 + lax.rem(q2 + d + R, R) * B2, B2), B2)

    def rows_b(t, d):
        return pl.ds(pl.multiple_of(row0(t) + lax.rem(q1 + d + R, R) * B1, B1), B1)

    def same(rows, cols, ss, rs, dev):
        return rc(stage_ref.at[rows, cols], stage_ref.at[rows, cols], ss, rs, dev)

    def sl(t):
        return lax.rem(t, 8)

    def aga1(t):
        s, r = sl(t), rows_a(t, 0)
        return (rc(yrow, stage_ref.at[r, :], aga_s.at[s, 0], aga_r.at[s, 0], plus2),
                rc(yrow, stage_ref.at[r, :], aga_s.at[s, 1], aga_r.at[s, 1], minus2))

    def aga2(t):
        s = sl(t)
        return (same(rows_a(t, -1), DA, aga_s.at[s, 2], aga_r.at[s, 2], plus2),
                same(rows_a(t, 1), DB, aga_s.at[s, 3], aga_r.at[s, 3], minus2))

    def agb1(t, r):
        s, rows, k = sl(t), rows_a(t, r), 2 * (r % R)
        src = yrow if r == 0 else stage_ref.at[rows, :]
        return (rc(src, stage_ref.at[rows, :], agb_s.at[s, k], agb_r.at[s, k], plus1),
                rc(src, stage_ref.at[rows, :], agb_s.at[s, k + 1], agb_r.at[s, k + 1], minus1))

    def agb2(t):
        s = sl(t)
        return (same(rows_b(t, -1), DA, agb_s.at[s, 8], agb_r.at[s, 8], plus1),
                same(rows_b(t, 1), DB, agb_s.at[s, 9], agb_r.at[s, 9], minus1))

    def dd(t, r):
        s, k = lax.rem(t, 8), r % R
        return (same(rows_b(t, r), pl.ds(0, D), dd_s.at[s, k], dd_r.at[s, k], mate),)

    def yloc(t):
        return pltpu.make_async_copy(yrow, stage_ref.at[rows_a(t, 0), :], loc_sem.at[0])

    def xload(t):
        return pltpu.make_async_copy(x_ref.at[rows_a(t, 0), :], xrow, loc_sem.at[1])

    def start(cs):
        for cp in cs:
            cp.start()

    def wrecv(cs):
        for cp in cs:
            cp.wait_recv()

    def wsend(cs):
        for cp in cs:
            cp.wait_send()

    def comb(src, q, rows, lf, ld, sm, dst):
        sm[0] = src[blk(q, 1, rows), A] + lf[0]
        sm[1] = src[blk(q, -1, rows), B] + lf[1]
        dst[:, A] = src[blk(q, 0, rows), A] + ld[1]
        dst[:, B] = src[blk(q, 0, rows), B] + ld[0]

    def e1(t):
        wrecv(p1s1(t))
        wsend(p1s1(t))

        @pl.when(t >= 1)
        def _():
            wsend(p1s2(t - 1))
        comb(r0, q1, B1, l1f, l1d, s1, r1.at[lax.rem(t, 2)])
        start(p1s2(t))

    def e2(t):
        s = lax.rem(t, 2)
        wrecv(p1s2(t))
        r1[s, :, A] = r1[s, :, A] + l1s[0]
        r1[s, :, B] = r1[s, :, B] + l1s[1]
        start(p2s1(t))

    def e3(t):
        s = lax.rem(t, 2)
        wrecv(p2s1(t))
        wsend(p2s1(t))

        @pl.when(t >= 1)
        def _():
            wsend(p2s2(t - 1))
        comb(r1.at[s], q2, B2, l2f.at[s], l2d.at[s], s2, r2)
        start(p2s2(t))
        xload(t).start()

    def e4(t):
        s = lax.rem(t, 2)
        wrecv(p2s2(t))
        xload(t).wait()
        i = ids_ref[t // tps]
        r2[:, A] = r2[:, A] + l2s[s, 0]
        r2[:, B] = r2[:, B] + l2s[s, 1]
        lor = jnp.dot(r2[:, pl.ds(D, W - D)], bod_v[i], preferred_element_type=jnp.float32)
        y = xrow[...].astype(jnp.float32) + r2[:, pl.ds(0, D)].astype(jnp.float32) + scale * lor
        yrow[...] = y.astype(BF)
        yloc(t).start()
        start(aga1(t))
        start(agb1(t, 0))

    def e5(t):
        yloc(t).wait()
        wsend(aga1(t))
        wsend(agb1(t, 0))
        wrecv(aga1(t))
        start(aga2(t))
        start(agb1(t, -1))
        start(agb1(t, 1))

    def e6(t):
        wrecv(aga2(t))
        start(agb1(t, 2))
        start(dd(t, 0))

    def e7(t):
        for r in (0, -1, 1, 2):
            wrecv(agb1(t, r))
        start(agb2(t))
        start(dd(t, -1))
        start(dd(t, 1))
        for r in (-1, 1, 2):
            wsend(agb1(t, r))
        wsend(aga2(t))

    def e8(t):
        wrecv(agb2(t))
        start(dd(t, 2))

    def e9(t):
        for r in (0, -1, 1, 2):
            wrecv(dd(t, r))
            wsend(dd(t, r))
        wsend(agb2(t))

    F32 = jnp.float32

    def pn(t, hf):
        u = 2 * t + hf
        settle(t, hf, 0)
        xcopy(u).wait()

        @pl.when(u + 1 < 2 * NT)
        def _():
            xcopy(u + 1).start()
        s = lax.rem(u, 2)
        RB = 16

        def step(k, _):
            rows = pl.ds(pl.multiple_of(k * RB, RB), RB)
            xf = xbuf[s, rows, :].astype(F32)
            inv = lax.rsqrt(jnp.sum(xf * xf, axis=-1, keepdims=True) * (1.0 / D) + EPS)
            hbuf[rows, :] = (xf * inv * gain_v[...]).astype(BF)
            return 0
        lax.fori_loop(0, HALF // RB, step, 0, unroll=8)

    def nt(a, b):
        return lax.dot_general(a, b, (((1,), (1,)), ((), ())), preferred_element_type=F32)

    def pm(t, hf):
        i = ids_ref[t // tps]
        n = at_v.shape[1]
        both = at_v[pl.ds(2 * i, 2)].reshape(2 * n, D)
        mids[:, pl.ds(0, 2 * n)] = nt(hbuf[...], both).astype(BF)
        mids[:, pl.ds(2 * n, n)] = nt(hbuf[...], at_v[at_v.shape[0] - 1]).astype(BF)

    def rope(z, rows):
        return z * cos_v[rows, :] + pltpu.roll(z, HEAD // 2, 1) * sin_v[rows, :]

    def pb(t, hf):
        settle(t, hf, 1)
        i = ids_ref[t // tps]
        pos = pl.ds(pl.multiple_of(lax.rem(t, tps) * TT + hf * HALF, HALF), HALF)
        z = jnp.dot(hbuf[...], wqkv_v[...], preferred_element_type=F32)
        n = at_v.shape[1]
        lqk = jnp.dot(mids[:, pl.ds(0, n)], bin_v[i, :, pl.ds(0, 2 * HEAD)], preferred_element_type=F32)
        lv = jnp.dot(mids[:, pl.ds(2 * n, n)], bin_v[i, :, pl.ds(2 * HEAD, HEAD)], preferred_element_type=F32)
        qbuf[...] = rope(z[:, :HEAD] + scale * lqk[:, :HEAD], pos).astype(BF)
        kbuf[pos, :] = rope(z[:, HEAD:2 * HEAD] + scale * lqk[:, HEAD:], pos).astype(BF)
        vbuf[pos, :] = (z[:, 2 * HEAD:] + scale * lv).astype(BF)

    def pc(t, hf):
        settle(t, hf, 2)
        i = ids_ref[t // tps]
        for n in range(FF // FB):
            cols = pl.ds(n * 2 * FB, 2 * FB)
            z = jnp.dot(hbuf[...], wgu_v[:, cols], preferred_element_type=F32)
            z = z + scale * jnp.dot(mids[:, pl.ds(at_v.shape[1], at_v.shape[1])], bin_v[i, :, pl.ds(3 * HEAD + n * 2 * FB, 2 * FB)], preferred_element_type=F32)
            g = z[:, :FB]
            om[lax.rem(t, 2), hf, :, pl.ds(HEAD + n * FB, FB)] = (g * (1.0 / (1.0 + jnp.exp(-g))) * z[:, FB:]).astype(BF)

    def pd(t, hf):
        sc = lax.dot_general(qbuf[...], kbuf[...], (((1,), (1,)), ((), ())), preferred_element_type=F32) * (1.0 / math.sqrt(HEAD))
        row = lax.rem(t, tps) * TT + hf * HALF + lax.broadcasted_iota(jnp.int32, (HALF, KV), 0)
        col = lax.broadcasted_iota(jnp.int32, (HALF, KV), 1)
        sc = jnp.where(row >= col, sc, -1e30)
        e = jnp.exp(sc - jnp.max(sc, axis=-1, keepdims=True))
        p = (e / jnp.sum(e, axis=-1, keepdims=True)).astype(BF)
        om[lax.rem(t, 2), hf, :, pl.ds(0, HEAD)] = jnp.dot(p, vbuf[...], preferred_element_type=F32).astype(BF)

    def out_proj(t, half, dst, extra, hooks):
        i = ids_ref[t // tps]
        act = om[lax.rem(t, 2), half]
        NB = 512
        for n in range(D // NB + 1):
            cols = pl.ds(n * NB, min(NB, W - n * NB))
            if n in hooks:
                hooks[n]()
            w = wod_v[:, cols] if n < D // NB else aod_v[i]
            acc = jnp.dot(act, w, preferred_element_type=F32)
            dst[:, cols] = (acc if extra is None else acc + extra[:, cols].astype(F32)).astype(BF)

    def pf(t):
        settle(t, 0, 3)

        @pl.when(t >= 1)
        def _():
            wsend(d2d(t - 1))
        out_proj(t, 1 - c, psend, None, {5: lambda: d2d(t)[0].start()})
        d2d(t)[1].start()

    def pg(t):
        out_proj(t, c, r0, l0.at[lax.rem(t, 2)], {0: lambda: d2d(t)[0].wait_recv(), 4: lambda: d2d(t)[1].wait_recv(),
                                                 5: lambda: start(p1s1(t)[0::3])})
        start(p1s1(t)[1:3])

    def guard(t, f, *a):
        @pl.when(jnp.logical_and(t >= 0, t < NT))
        def _():
            f(t, *a)

    def piece(ad, d, k, dev):
        ref = bod_v.at[ad, :, bcols(d)] if ad is not None else bod_v.at[:, :, bcols(d)]
        return rc(ref, ref, bg_s.at[k], bg_r.at[k], dev)

    def line(dev, k):
        return dev + (k - q2) * st2

    def g1():
        return (piece(None, idx, 0, plus2), piece(None, idx, 1, minus2))

    def g2():
        return (piece(0, minus2, 2, plus2), piece(1, plus2, 3, minus2))

    def g3():
        return tuple(piece(None, line(idx, k), 4 + k, plus1) for k in range(R)) + tuple(piece(None, line(idx, k), 4 + R + k, minus1) for k in range(R))

    def g4():
        return tuple(piece(0, line(minus1, k), 4 + 2 * R + k, plus1) for k in range(R)) + tuple(piece(1, line(plus1, k), 4 + 3 * R + k, minus1) for k in range(R))

    def g5():
        return tuple(piece(None, 2 * j + c, 4 + 4 * R + j, mate) for j in range(R * R))

    def b1():
        for cp in bown:
            cp.wait()
        start(g1())

    def b2():
        wrecv(g1())
        start(g2())

    def b3():
        wrecv(g2())
        start(g3())

    def b4():
        wrecv(g3())
        start(g4())

    def b5():
        wrecv(g4())
        start(g5())

    def b6():
        for g in (g1, g2, g3, g4, g5):
            wsend(g())
        wrecv(g5())

    def at_step(it, k, f):
        @pl.when(it == k)
        def _():
            f()

    def ln(dev, r):
        return dev - q2 * st2 + lax.rem(q2 + r + R, R) * st2

    def arow(d, k, dev, cols):
        ref = at_v.at[:, arows(d), cols]
        return rc(ref, ref, ag_s.at[k], ag_r.at[k], dev)

    full = pl.ds(0, D)
    opp1 = base1 + lax.rem(q1 + 2, R) * st1
    lines = (idx, minus1, plus1, opp1)

    def a1():
        return (arow(idx, 0, plus2, full), arow(idx, 1, minus2, full))

    def a2():
        return (arow(minus2, 2, plus2, DA), arow(plus2, 3, minus2, DB))

    def ab(r):
        return (arow(ln(idx, r), 4 + r % R, plus1, full), arow(ln(idx, r), 4 + R + r % R, minus1, full))

    def af(r):
        return (arow(ln(minus1, r), 4 + 2 * R + r % R, plus1, DA), arow(ln(plus1, r), 4 + 3 * R + r % R, minus1, DB))

    def am(j, r):
        return (arow(ln(lines[j], r), 4 + 4 * R + R * j + r % R, mate, full),)

    def weave():
        for cp in bload:
            cp.wait()
        n = bin_v.shape[1]
        part = AR // 2
        row = lax.broadcasted_iota(jnp.int32, (n, RANK), 0)
        col = lax.broadcasted_iota(jnp.int32, (n, RANK), 1)
        picks = [jnp.where(row == (col // part) * AR + part * k + lax.rem(col, part), 1.0, 0.0).astype(BF) for k in range(2)]
        for ad in range(bin_v.shape[0]):
            for _, at, width, _, kind in bcol:
                pick = picks[ad if kind == 2 else kind]
                bin_v[ad, :, pl.ds(at, width)] = jnp.dot(pick, bst_v[ad, :, pl.ds(at, width)], preferred_element_type=F32).astype(BF)

    def gather_a():
        for cp in aown:
            cp.wait()
        start(a1())
        start(ab(0))
        start(am(0, 0))
        pn(0, 0)
        wrecv(a1())
        start(a2())
        for r in (-1, 1):
            start(ab(r))
            start(am(0, r))
        wrecv(a2())
        start(ab(2))
        start(am(0, 2))
        weave()
        for r in (0, -1, 1, 2):
            wrecv(ab(r))
            start(af(r))
            start(am(1, r))
            start(am(2, r))
        for r in (0, -1, 1, 2):
            wrecv(af(r))
            start(am(3, r))
        for j in range(4):
            for r in (0, -1, 1, 2):
                wrecv(am(j, r))
        wsend(a1())
        wsend(a2())
        for r in (0, -1, 1, 2):
            wsend(ab(r))
            wsend(af(r))
            for j in range(4):
                wsend(am(j, r))

    gather_a()
    b1()

    def body(it, _):
        at_step(it, 3, b6)
        guard(it - 3, e4)
        guard(it - 8, e9)
        @pl.when(jnp.logical_and(it >= 1, it < NT))
        def _():
            pn(it, 0)
        guard(it - 2, e2)
        guard(it, pm, 0)
        guard(it - 1, pg)
        at_step(it, 0, b2)
        at_step(it, 1, b4)
        guard(it, pb, 0)
        guard(it - 3, e5)
        guard(it, pc, 0)
        guard(it - 7, e8)
        guard(it, pd, 0)
        guard(it, pn, 1)
        guard(it, pm, 1)
        guard(it - 2, e3)
        guard(it, pb, 1)
        guard(it - 1, e1)
        guard(it - 5, e7)
        at_step(it, 0, b3)
        at_step(it, 1, b5)
        guard(it, pc, 1)
        guard(it - 3, e6)
        guard(it, pd, 1)
        guard(it, pf)
        return 0
    lax.fori_loop(0, NT + 8, body, 0)
    last = NT - 1
    wsend(d2d(last))
    wsend(p1s2(last))
    wsend(p2s2(last))


def fused(mesh, ids, x, gain, aown, avown, wq, wk, wv, wg, wu, wo, wd, bq, bk, bv, bg, bu, ao, ad, bo, bd, cos, sin, scale, seq_len, TT):
    R = math.isqrt(mesh.shape["tensor"] // 2)
    T, D = x.shape
    HEAD, FF = wo.shape[0], wd.shape[0]
    W = D + 2 * ao.shape[-1]
    NT, HALF = T // TT, TT // 2
    B1 = HALF // R
    B2 = B1 // R
    WH = W // 2
    cfg = (R, NT, TT, W, D, HEAD, FF, scale, seq_len // TT)
    S = pltpu.SemaphoreType.DMA

    def V(*shape):
        return pltpu.VMEM(shape, BF)
    n_in = 22
    n_ad, rank = bq.shape[:2]
    b_cols = 3 * HEAD + 2 * FF
    rows_a = aown.shape[1] * mesh.shape["tensor"]
    return pl.pallas_call(
        functools.partial(fused_kernel, cfg), name="block",
        out_shape=jax.ShapeDtypeStruct((T, D), BF),
        in_specs=[pl.BlockSpec(memory_space=pltpu.SMEM)] + [pl.BlockSpec(memory_space=pltpu.HBM)] * n_in,
        out_specs=pl.BlockSpec(memory_space=pltpu.HBM),
        scratch_shapes=[V(2, HALF, D), V(HALF, D), V(HALF, 3 * rows_a), pltpu.VMEM(gain.shape, jnp.float32), V(aown.shape[0] + 1, rows_a, D), V(D, 3 * HEAD), V(D, 2 * FF), V(HEAD + FF, D),
                        V(n_ad, rank, b_cols), V(n_ad, rows_a, b_cols), V(ao.shape[0], HEAD + FF, W - D), V(bo.shape[0], W - D, D),
                        pltpu.VMEM(cos.shape, jnp.float32), pltpu.VMEM(sin.shape, jnp.float32), V(HALF, HEAD), V(seq_len, HEAD), V(seq_len, HEAD), V(2, 2, HALF, HEAD + FF),
                        V(HALF, W), V(2, HALF, W), V(HALF, W),
                        V(2, B1, WH), V(2, B1, WH), V(2, B1, WH), V(2, B1, WH), V(2, B1, W),
                        V(2, 2, B2, WH), V(2, 2, B2, WH), V(2, 2, B2, WH), V(2, B2, WH), V(B2, W),
                        V(B2, D), V(B2, D),
                        S((14,)), S((2,)), S((2,)), S((2, 2)), S((6,)), S((6,)), S((2, 6)), S((2, 6)), S((8, 4)), S((8, 4)), S((8, 10)), S((8, 10)), S((8, 4)), S((8, 4)), S((4 + 8 * R,)), S((4 + 8 * R,)), S((4 + 4 * R + R * R,)), S((4 + 4 * R + R * R,)), S((6 + 3 + 2 * (2 * FF // TT),))],
        compiler_params=pltpu.CompilerParams(collective_id=0, has_side_effects=True, vmem_limit_bytes=67043328),
    )(ids, x, gain, aown, avown, wq, wk, wv, wg, wu, wo, wd, bq, bk, bv, bg, bu, ao, ad, bo, bd, cos, sin)


def solution(mesh):
    batch_spec = P('data', None, None)
    head_cols = P(None, 'tensor', None)
    head_rows = P('tensor', None, None)
    ff_cols = P(None, 'tensor')
    ff_rows = P('tensor', None)
    last_split = P(None, None, 'tensor')
    b_heads = P(None, None, 'tensor', None)
    a_heads = P(None, 'tensor', None, None)
    in_specs = (batch_spec, P('data'), P(None), head_cols, head_cols, head_cols, head_rows, ff_cols, ff_cols, ff_rows, last_split, b_heads, last_split, b_heads, last_split, b_heads, a_heads, last_split, last_split, last_split, last_split, last_split, head_cols, last_split)

    def local_layer(x_blk, adapter_ids, norm_gain, w_query, w_key, w_value, w_out, w_gate, w_up, w_down, a_query, b_query, a_key, b_key, a_value, b_value, a_out, b_out, a_gate, b_gate, a_up, b_up, a_down, b_down):
        seq_len = x_blk.shape[1]
        rank = a_out.shape[-1]
        scale = ALPHA / rank
        dim = x_blk.shape[2]
        n_ad = a_query.shape[0]
        zero_a = jnp.zeros_like(a_value)
        by_rank = [jnp.transpose(st, (0, 2, 1)) for st in (a_query, a_key, a_gate, a_up)]
        mine = jnp.concatenate(by_rank, axis=1).reshape(2 * n_ad, -1, dim)
        mine_v = jnp.transpose(a_value, (0, 2, 1)).reshape(1, -1, dim)
        head = w_query.shape[-1]
        tile = seq_len // 2

        def flat(b_stack):
            return b_stack.reshape(n_ad, rank, head)

        half = head // 2
        inv_freq = np.float32(ROPE_BASE) ** (-np.arange(half, dtype=np.float32) / np.float32(half))
        angles = np.arange(seq_len, dtype=np.float32)[:, None] * inv_freq[None, :]
        cos_t, sin_t = np.cos(angles), np.sin(angles)
        cos_t = jnp.asarray(np.concatenate([cos_t, cos_t], axis=1))
        sin_t = jnp.asarray(np.concatenate([-sin_t, sin_t], axis=1))
        out = fused(mesh, adapter_ids, x_blk.reshape(-1, dim), norm_gain.reshape(1, dim), mine, mine_v, w_query.reshape(dim, head), w_key.reshape(dim, head), w_value.reshape(dim, head),
                    w_gate, w_up, w_out.reshape(head, dim), w_down, flat(b_query), flat(b_key), flat(b_value), b_gate, b_up, a_out.reshape(n_ad, head, rank), a_down, b_out, b_down, cos_t, sin_t, scale, seq_len, tile)
        return out.reshape(x_blk.shape)

    return jax.shard_map(local_layer, mesh=mesh, in_specs=in_specs, out_specs=batch_spec, check_vma=False)
```
